32 devices in a mesh: fsdp: 4 (over y, core), sp: 8 (over z, x).
Axes of the slice: x: 2, y: 2, z: 4, core: 2. Of those that a mesh axis runs over, the one named last changes fastest.
Arguments:
- hidden: bfloat16 [2048, 8192], P('sp', 'fsdp'), may hold values from -23 to 23
- w_query: bfloat16 [8192, 1024], P('fsdp', 'sp'), may hold values from -0.125 to 0.125
- w_keyvalue: bfloat16 [8192, 256], P('fsdp', 'sp'), may hold values from -0.125 to 0.125
- w_output: bfloat16 [1024, 8192], P('sp', 'fsdp'), may hold values from -0.75 to 0.75
- segment_ids: int32 [2048], P('sp'), may hold values from 0 to 7, never falling along the last dimension, each value on 1 to 512 neighbouring positions
Outputs:
- attended: bfloat16 [2048, 8192], P('sp', 'fsdp')
The draws below stay inside these ranges and needn't reach their ends.
Inputs may be any that keep to these rules, and one draw needn't show every extreme that they name: `segment_ids`: segment ids never fall along the sequence; every episode has between 1 and 512 tokens.
All inputs are finite; a program needn't handle non-finite values.
Results may differ from the reference program's by a relative error of at most 0.0085.
The reference program's roundings to bfloat16 on the way count: a program that leaves them out, or rounds other values in their place, can miss the bound.
Values may be sent and summed in bfloat16 or wider, within the bound.
A program may use at most 128 MiB of HBM per device.

```python
import math
import jax
import jax.numpy as jnp
import numpy as np
from jax import lax

D = 8192
HD = 128
GROUP = 8
HEADS = 8
KV_HEADS = 1
SEQ = 2048


def draw_hidden(key, part):
    base_key = jax.random.fold_in(jax.random.fold_in(key, 11), 0)
    entries = jnp.clip(jax.random.normal(base_key, (SEQ, D), jnp.float32), -6.0, 6.0)
    return entries.astype(jnp.bfloat16)


def steps_of(own_key, shape, pieces, low, largest):
    def one(position, blocks):
        heights = jax.random.uniform(jax.random.fold_in(jax.random.fold_in(own_key, 6), position), (blocks,), jnp.float32, low / len(pieces), largest / len(pieces))
        return jnp.repeat(jnp.exp(heights), shape[position] // blocks).reshape((-1,) + (1,) * (len(shape) - position - 1))

    loudness = one(*pieces[0])
    for cut in pieces[1:]:
        loudness = loudness * one(*cut)
    return loudness


def profile(count, total, limit, slope):
    weights = [(1 << 20) // math.isqrt(grade ** slope) + 1 for grade in range(2, count + 1)]
    surplus, holding = total - limit - (count - 1), [1] * (count - 1)
    while surplus > 0:
        candidates = [i for i in range(count - 1) if holding[i] < limit]
        pool, remaining = sum([weights[i] for i in candidates]), surplus
        for i in candidates:
            addition = min(limit - holding[i], max(1, remaining * weights[i] // pool), surplus)
            holding[i] = holding[i] + addition
            surplus = surplus - addition
    return np.array([limit] + holding)


def ragged_sizes(own_key, number_of, total, reach, skew):
    if number_of == 2:
        one = jax.random.randint(own_key, (), max(1, total - reach), min(reach, total - 1) + 1)
        return jnp.stack([one, total - one])
    lengths = jnp.asarray(profile(number_of, total, reach, skew), jnp.int32)
    couples = (number_of - 1) // 2
    source_of, sink = lengths[1:1 + 2 * couples:2], lengths[2:2 + 2 * couples:2]
    room = jnp.minimum(source_of - 1, reach - sink)
    shifted = jax.random.randint(jax.random.fold_in(own_key, 1), (couples,), 0, 1 << 20) % (room + 1)
    lengths = lengths.at[1:1 + 2 * couples:2].set(source_of - shifted).at[2:2 + 2 * couples:2].set(sink + shifted)
    return lengths[jax.random.permutation(jax.random.fold_in(own_key, 2), number_of)]


def scatter_about(own_key, dims, spread, bound, pieces=(), held_as=jnp.bfloat16):
    values = jax.random.normal(own_key, dims, jnp.float32) * spread
    if len(pieces) > 0:
        values = steps_of(own_key, dims, pieces, -0.22, 0.18) * values
    return jnp.clip(values, min=-bound, max=bound).astype(held_as)


def setup_inputs(seed: int = 0) -> dict:
    arg_keys = jax.random.split(jax.random.key(seed), 6)
    return {
        "hidden": draw_hidden(jax.random.fold_in(arg_keys[5], 71), 0),
        "w_query": scatter_about(arg_keys[1], (D, HEADS * HD), (D // 4) ** -0.5, 0.125, ((0, 4), (1, 8))),
        "w_keyvalue": scatter_about(arg_keys[2], (D, 2 * KV_HEADS * HD), (D // 4) ** -0.5, 0.125, ((0, 4), (1, 8))),
        "w_output": scatter_about(arg_keys[3], (HEADS * HD, D), (HEADS * HD // 16) ** -0.5, 0.75, ((0, 8), (1, 4))),
        "segment_ids": jnp.searchsorted(jnp.cumsum(ragged_sizes(arg_keys[4], 8, SEQ, SEQ // 4, 0)), jnp.arange(SEQ), side="right").astype(jnp.int32),
    }


ROPE_BASE = 500000.0
NEG_FILL = -1.0e30


def rotate(values, positions, head_count, width):
    row_count = values.shape[0]
    shaped = values.reshape(row_count, head_count, width)
    half_width = width // 2
    frequency = jnp.exp(jnp.arange(half_width, dtype=jnp.float32) * (-2.0 * math.log(ROPE_BASE) / width))
    angles = positions.astype(jnp.float32)[:, None] * frequency[None, :]
    cosine = jnp.cos(angles)[:, None, :]
    sine_part = jnp.sin(angles)[:, None, :]
    lower_half = shaped[:, :, :half_width]
    upper_half = shaped[:, :, half_width:]
    turned = jnp.concatenate([lower_half * cosine - upper_half * sine_part, upper_half * cosine + lower_half * sine_part], axis=2)
    return turned.reshape(row_count, head_count * width)


def split_keys(kv_sum, positions, kv_count, width):
    row_count = kv_sum.shape[0]
    shaped = kv_sum.reshape(row_count, kv_count, 2, width)
    key_part = rotate(shaped[:, :, 0, :].reshape(row_count, kv_count * width), positions, kv_count, width)
    key_part = key_part.reshape(row_count, kv_count, 1, width)
    return jnp.concatenate([key_part, shaped[:, :, 1:2, :]], axis=2).astype(jnp.bfloat16)


def reference(hidden, w_query, w_keyvalue, w_output, segment_ids):
    seq_len = hidden.shape[0]
    positions = jnp.arange(seq_len, dtype=jnp.int32)
    query = rotate(jnp.dot(hidden, w_query, preferred_element_type=jnp.float32), positions, HEADS, HD).astype(jnp.bfloat16)
    pairs = split_keys(jnp.dot(hidden, w_keyvalue, preferred_element_type=jnp.float32), positions, KV_HEADS, HD)
    key_all = pairs[:, :, 0, :]
    value_all = pairs[:, :, 1, :]
    block_len = min(512, seq_len)
    block_count = seq_len // block_len
    score_scale = HD ** -0.5

    def one_block(item_index):
        head_id = item_index // block_count
        block_id = item_index % block_count
        first_row = (block_id * block_len).astype(jnp.int32)
        query_block = lax.dynamic_slice(query, (first_row, (head_id * HD).astype(jnp.int32)), (block_len, HD))
        group_id = (head_id // GROUP).astype(jnp.int32)
        key_block = lax.dynamic_index_in_dim(key_all, group_id, axis=1, keepdims=False)
        value_block = lax.dynamic_index_in_dim(value_all, group_id, axis=1, keepdims=False)
        scores = lax.dot_general(query_block, key_block, (((1,), (1,)), ((), ())), preferred_element_type=jnp.float32) * score_scale
        query_pos = first_row + jnp.arange(block_len, dtype=jnp.int32)
        query_seg = lax.dynamic_slice_in_dim(segment_ids, first_row, block_len)
        allowed = (positions[None, :] <= query_pos[:, None]) & (segment_ids[None, :] == query_seg[:, None])
        masked = jnp.where(allowed, scores, NEG_FILL)
        row_max = jnp.max(masked, axis=1, keepdims=True)
        weights = jnp.where(allowed, jnp.exp(masked - row_max), 0.0)
        row_total = jnp.sum(weights, axis=1, keepdims=True)
        mixed_block = jnp.dot(weights.astype(jnp.bfloat16), value_block, preferred_element_type=jnp.float32)
        return (mixed_block / row_total).astype(jnp.bfloat16)

    blocks = lax.map(one_block, jnp.arange(HEADS * block_count, dtype=jnp.int32))
    mixed = blocks.reshape(HEADS, seq_len, HD).transpose(1, 0, 2).reshape(seq_len, HEADS * HD)
    return jnp.dot(mixed, w_output, preferred_element_type=jnp.float32).astype(jnp.bfloat16)
```

```python
import functools
import math

import jax
import jax.numpy as jnp
from jax import lax
from jax.experimental import pallas as pl
from jax.experimental.pallas import tpu as pltpu
from jax.sharding import PartitionSpec as P

HD = 128
GROUP = 8


ROPE_BASE = 500000.0
NEG_FILL = -1e30


def rotate(values, positions, head_count, width):
    row_count = values.shape[0]
    shaped = values.reshape(row_count, head_count, width)
    half_width = width // 2
    frequency = jnp.exp(
        jnp.arange(half_width, dtype=jnp.float32) * (-2.0 * math.log(ROPE_BASE) / width)
    )
    angles = positions.astype(jnp.float32)[:, None] * frequency[None, :]
    cosine = jnp.cos(angles)[:, None, :]
    sine_part = jnp.sin(angles)[:, None, :]
    lower_half = shaped[:, :, :half_width]
    upper_half = shaped[:, :, half_width:]
    turned = jnp.concatenate(
        [
            lower_half * cosine - upper_half * sine_part,
            upper_half * cosine + lower_half * sine_part,
        ],
        axis=2,
    )
    return turned.reshape(row_count, head_count * width)


def split_keys(kv_sum, positions, kv_count, width):
    row_count = kv_sum.shape[0]
    shaped = kv_sum.reshape(row_count, kv_count, 2, width)
    key_part = rotate(
        shaped[:, :, 0, :].reshape(row_count, kv_count * width), positions, kv_count, width
    )
    key_part = key_part.reshape(row_count, kv_count, 1, width)
    return jnp.concatenate([key_part, shaped[:, :, 1:2, :]], axis=2).astype(jnp.bfloat16)


def merge_keys(
    state_in, query_tile, query_pos_tile, query_seg_tile, key_tile, key_pos_tile, key_seg_tile
):
    running_max, running_sum, weighted = state_in
    allowed = (key_pos_tile[None, :] <= query_pos_tile[:, None]) & (
        key_seg_tile[None, :] == query_seg_tile[:, None]
    )
    key_part = key_tile[:, :HD]
    value_part = key_tile[:, HD:]
    scores = lax.dot_general(
        query_tile, key_part, (((1,), (1,)), ((), ())), preferred_element_type=jnp.float32
    ) * HD ** (-0.5)
    masked = jnp.where(allowed, scores, NEG_FILL)
    new_max = jnp.maximum(running_max, jnp.max(masked, axis=1))
    weights = jnp.where(allowed, jnp.exp(masked - new_max[:, None]), 0.0)
    new_sum = jnp.sum(weights, axis=1)
    new_weighted = jnp.dot(
        weights.astype(jnp.bfloat16), value_part, preferred_element_type=jnp.float32
    )
    return (new_max, new_sum, new_weighted)


def on_device(hidden, w_query, w_keyvalue, w_output, segment_ids):
    fsdp_count = lax.axis_size("fsdp")
    seq_count = lax.axis_size("sp")
    fsdp_index = lax.axis_index("fsdp")
    seq_index = lax.axis_index("sp")
    tok_rows = hidden.shape[0]
    sub_rows = tok_rows // fsdp_count
    kv_count = seq_count // GROUP
    query_rows = seq_count * sub_rows
    offsets = jnp.arange(query_rows, dtype=jnp.int32)
    query_pos = offsets // sub_rows * tok_rows + fsdp_index * sub_rows + offsets % sub_rows
    own_positions = (
        seq_index * tok_rows + fsdp_index * sub_rows + jnp.arange(sub_rows, dtype=jnp.int32)
    )

    def project(weight_block):
        return jnp.dot(hidden, weight_block, preferred_element_type=jnp.float32)

    query_part = project(lax.all_gather(w_query, "sp", axis=1, tiled=True))
    kv_part = project(lax.all_gather(w_keyvalue, "sp", axis=1, tiled=True))
    query_sum, kv_sum = (
        lax.psum_scatter(query_part, "fsdp", scatter_dimension=0, tiled=True),
        lax.psum_scatter(kv_part, "fsdp", scatter_dimension=0, tiled=True),
    )
    query_local = rotate(query_sum, own_positions, seq_count, HD).astype(jnp.bfloat16)
    pairs = split_keys(kv_sum, own_positions, kv_count, HD)
    expanded = jnp.repeat(pairs, GROUP, axis=1).reshape(sub_rows, seq_count * 2 * HD)
    query_head, kv_head = (
        lax.all_to_all(query_local, "sp", split_axis=1, concat_axis=0, tiled=True),
        lax.all_to_all(expanded, "sp", split_axis=1, concat_axis=0, tiled=True),
    )
    segment_all = lax.all_gather(segment_ids, "sp", axis=0, tiled=True)
    query_seg = segment_all[query_pos]
    initial = (
        jnp.full((query_rows,), NEG_FILL, jnp.float32),
        jnp.zeros((query_rows,), jnp.float32),
        jnp.zeros((query_rows, HD), jnp.float32),
    )
    block_keys = lax.all_gather(kv_head, "fsdp", axis=0, tiled=True)
    piece_rows = block_keys.shape[0]
    row_ids = jnp.arange(piece_rows, dtype=jnp.int32)
    source_id = row_ids // query_rows
    within = row_ids % query_rows
    key_pos = within // sub_rows * tok_rows + source_id * sub_rows + within % sub_rows
    key_seg = segment_all[key_pos]
    final_max, final_sum, final_weighted = merge_keys(
        initial, query_head, query_pos, query_seg, block_keys, key_pos, key_seg
    )
    attention = (final_weighted / final_sum[:, None]).astype(jnp.bfloat16)
    back_rows = lax.all_to_all(attention, "sp", split_axis=0, concat_axis=1, tiled=True)
    mixed_rows = lax.all_gather(back_rows, "fsdp", axis=0, tiled=True)
    result = jnp.dot(
        mixed_rows,
        lax.all_gather(w_output, "sp", axis=0, tiled=True),
        preferred_element_type=jnp.float32,
    )
    return result.astype(jnp.bfloat16)


NEG_POS = -1
WO_CHUNKS = 2


def fused_kernel(
    nf, nz, nx, hid, wq, wkv, wo, seg, out,
    h_buf, wq_buf, wkv_buf, wo_buf, seg_buf,
    q_part, q_recv, kv_part, kv_recv, kv_piece, kv_all, mix_own, mix_buf,
    s_loc, s_hid, r_hid, s_seg, r_seg, s_wkv, r_wkv, s_wqr, s_wql, r_wq,
    s_q, r_q, s_kvp, r_kvp, s_kv, r_kv, s_wor, s_wol, s_wox, r_wo, s_mix, r_mix,
):
    f = lax.axis_index("fsdp")
    s = lax.axis_index("sp")
    z, x = s // nx, s % nx
    tok, kdim = hid.shape
    rows = tok * nx
    sub = rows // nf
    kvw = wkv.shape[0]
    other = 1 - x
    chunk = wo.shape[1] // WO_CHUNKS
    f32, bf16 = jnp.float32, jnp.bfloat16

    def dev(ff, zz, xx):
        return (ff, zz * nx + xx)

    def remote(src, dst, ss, rs, target):
        return pltpu.make_async_remote_copy(
            src_ref=src, dst_ref=dst, send_sem=ss, recv_sem=rs,
            device_id=target, device_id_type=pl.DeviceIdType.MESH,
        )

    def tile(ref, count):
        return pl.ds(pl.multiple_of(ref * count, count), count)

    here = (f, s)
    own_h = pltpu.make_async_copy(hid, h_buf.at[tile(x, tok)], s_loc.at[0])
    own_wq = pltpu.make_async_copy(wq, wq_buf.at[z], s_loc.at[1])
    own_wkv = pltpu.make_async_copy(wkv, wkv_buf.at[tile(z, kvw)], s_loc.at[2])
    own_wo = pltpu.make_async_copy(wo, wo_buf.at[tile(s, HD)], s_loc.at[3])
    own_seg = pltpu.make_async_copy(seg, seg_buf.at[1, x], s_loc.at[4])
    hid_send = remote(hid, h_buf.at[tile(x, tok)], s_hid, r_hid, dev(f, z, other))

    def hid_wait():
        remote(hid, h_buf.at[tile(other, tok)], s_hid, r_hid, here).wait_recv()

    def wkv_send(d):
        zz = lax.rem(z + d, nz)
        return remote(
            wkv, wkv_buf.at[tile(z, kvw)], s_wkv.at[d - 1], r_wkv.at[z], dev(f, zz, x)
        )

    def wkv_wait(d):
        zz = lax.rem(z + d, nz)
        remote(
            wkv, wkv_buf.at[tile(zz, kvw)], s_wkv.at[d - 1], r_wkv.at[zz], here
        ).wait_recv()

    def wq_copy(src, j, to_right):
        sems = s_wqr if to_right else s_wql
        return remote(
            src, wq_buf.at[j], sems.at[j], r_wq.at[j],
            dev(f, z + 1 if to_right else z - 1, x),
        )

    def wo_slice(zz, xx, c):
        return wo_buf.at[tile(zz * nx + xx, HD), c * chunk : (c + 1) * chunk]

    def wo_src(j, c, own):
        return wo.at[:, c * chunk : (c + 1) * chunk] if own else wo_slice(j, x, c)

    def wo_copy(j, c, to_right, own=False):
        sems = s_wor if to_right else s_wol
        return remote(
            wo_src(j, c, own), wo_slice(j, x, c), sems.at[j, c], r_wo.at[j * nx + x, c],
            dev(f, z + 1 if to_right else z - 1, x),
        )

    def wo_cross(j, c, own=False):
        return remote(
            wo_src(j, c, own), wo_slice(j, x, c), s_wox.at[j, c], r_wo.at[j * nx + x, c],
            dev(f, z, other),
        )

    def wo_wait(j, xx, c):
        remote(
            wo_slice(j, xx, c), wo_slice(j, xx, c), s_wox.at[j, c], r_wo.at[j * nx + xx, c], here
        ).wait_recv()

    def wo_own(to_right):
        for c in range(WO_CHUNKS):
            wo_copy(z, c, to_right, own=True).start()

    seg_same = remote(seg, seg_buf.at[1, x], s_seg.at[0], r_seg.at[1, x], dev(f, z, other))

    def seg_next(xx):
        return remote(
            seg, seg_buf.at[0, x], s_seg.at[1 + xx], r_seg.at[0, x], dev(f, z + 1, xx)
        )

    for d in range(1, nz):
        wkv_send(d).start()

    @pl.when(z < nz - 1)
    def _():
        wq_copy(wq, z, True).start()

    @pl.when(z > 0)
    def _():
        wq_copy(wq, z, False).start()

    hid_send.start()
    seg_same.start()

    @pl.when(z < nz - 1)
    def _():
        for xx in range(nx):
            seg_next(xx).start()

    for copy in (own_h, own_wq, own_wkv, own_wo, own_seg):
        copy.start()

    @pl.when(z == 0)
    def _():
        wo_own(True)
        kv_all[0] = jnp.zeros(kv_all.shape[1:], bf16)
        seg_buf[0] = jnp.full(seg_buf.shape[1:], NEG_POS, jnp.int32)

    @pl.when(z == nz - 1)
    def _():
        wo_own(False)

    def table(row_count, first, lane_index):
        position = (first + lax.broadcasted_iota(jnp.int32, (row_count, HD), 0)).astype(f32)
        frequency = jnp.exp(lane_index.astype(f32) * (-2.0 * math.log(ROPE_BASE) / HD))
        return position * frequency

    lane = lax.broadcasted_iota(jnp.int32, (1, HD), 1)
    half = HD // 2
    quarter = half // nx
    kv_angle = table(sub, z * rows + f * sub, x * quarter + lane % quarter)
    is_key = lane < half
    kv_cos = jnp.where(is_key, jnp.cos(kv_angle), 1.0)
    kv_sin = jnp.where(is_key, jnp.sin(kv_angle), 0.0)
    kv_sin = jnp.where(lane < quarter, -kv_sin, kv_sin)

    def wq_step(d):
        @pl.when(z >= d)
        def _():
            j = z - d
            wq_copy(wq_buf.at[j], j, True).wait_recv()

            @pl.when(z < nz - 1)
            def _():
                wq_copy(wq_buf.at[j], j, True).start()

                @pl.when(z == d)
                def _():
                    wo_own(True)

        @pl.when(z + d < nz)
        def _():
            j = z + d
            wq_copy(wq_buf.at[j], j, False).wait_recv()

            @pl.when(z > 0)
            def _():
                wq_copy(wq_buf.at[j], j, False).start()

                @pl.when(z + d == nz - 1)
                def _():
                    wo_own(False)

    def q_send(j):
        return remote(q_part.at[j], q_recv.at[f], s_q.at[j], r_q.at[f], (j, s))

    def q_project(j):
        q_part[j] = jnp.dot(h_buf[...], wq_buf[j], preferred_element_type=f32)

        @pl.when(j != f)
        def _():
            q_send(j).start()

    def q_step(d):
        @pl.when(z >= d)
        def _():
            q_project(z - d)

        @pl.when(z + d < nz)
        def _():
            q_project(z + d)

    wq_step(1)
    own_h.wait()
    own_wq.wait()
    own_wkv.wait()
    hid_wait()
    for c in range(WO_CHUNKS):
        wo_cross(z, c, own=True).start()
    for d in range(1, nz):
        wkv_wait(d)
    kv_part[...] = lax.dot_general(
        h_buf[...], wkv_buf[...], (((1,), (1,)), ((), ())), preferred_element_type=f32
    )

    def kvp_send(d):
        ff = lax.rem(f + d, nf)
        return remote(
            kv_part.at[tile(ff, sub)], kv_recv.at[f], s_kvp.at[d - 1], r_kvp.at[f], (ff, s)
        )

    def kvp_wait(d):
        ff = lax.rem(f + d, nf)
        remote(
            kv_part.at[tile(ff, sub)], kv_recv.at[ff], s_kvp.at[d - 1], r_kvp.at[ff], here
        ).wait_recv()

    for d in range(1, nf):
        kvp_send(d).start()
    q_project(z)
    q_step(1)
    total = kv_part[tile(f, sub), :]
    for d in range(1, nf):
        kvp_wait(d)
        total = total + kv_recv[lax.rem(f + d, nf)]
    partner = jnp.where(
        lane < quarter, pltpu.roll(total, HD - quarter, 1), pltpu.roll(total, quarter, 1)
    )
    kv_piece[...] = (total * kv_cos + partner * kv_sin).astype(bf16)
    piece_rows = tile(f, sub)
    own_piece = pltpu.make_async_copy(kv_piece, kv_all.at[1, x, piece_rows], s_loc.at[5])
    own_piece.start()

    def kv_send(plane, dx, d):
        ff, xx = lax.rem(f + d, nf), lax.rem(x + dx, nx)
        return remote(
            kv_piece, kv_all.at[plane, x, piece_rows],
            s_kv.at[plane, dx, d], r_kv.at[plane, x, f], dev(ff, z + 1 - plane, xx),
        )

    def kv_wait(plane, dx, d):
        ff, xx = lax.rem(f + d, nf), lax.rem(x + dx, nx)
        remote(
            kv_piece, kv_all.at[plane, xx, tile(ff, sub)],
            s_kv.at[plane, dx, d], r_kv.at[plane, xx, ff], here,
        ).wait_recv()

    pairs = [(dx, d) for dx in range(nx) for d in range(nf)]
    for pair in pairs[1:]:
        kv_send(1, *pair).start()

    @pl.when(z < nz - 1)
    def _():
        for pair in pairs:
            kv_send(0, *pair).start()

    for d in range(2, nz):
        wq_step(d)
        q_step(d)

    def wo_side(j, to_right):
        for c in range(WO_CHUNKS):
            wo_wait(j, x, c)
            if to_right is not None:
                wo_copy(j, c, to_right).start()
            wo_cross(j, c).start()

    def wo_mid(d):
        @pl.when((z >= d) & (z < nz - 1))
        def _():
            wo_side(z - d, True)

        @pl.when((z + d < nz) & (z > 0))
        def _():
            wo_side(z + d, False)

    def wo_end(d):
        if d < nz:
            @pl.when((z >= d) & (z == nz - 1))
            def _():
                wo_side(z - d, None)

            @pl.when((z + d < nz) & (z == 0))
            def _():
                wo_side(z + d, None)

    for d in range(1, nz - 1):
        wo_mid(d)

    q_angle = table(rows, z * rows, lane % half)
    q_cos = jnp.cos(q_angle)
    q_sin = jnp.where(lane < half, -jnp.sin(q_angle), jnp.sin(q_angle))
    q_total = q_part[f]
    for d in range(1, nf):
        ff = lax.rem(f + d, nf)
        remote(q_part.at[0], q_recv.at[ff], s_q.at[0], r_q.at[ff], here).wait_recv()
        q_total = q_total + q_recv[ff]
    q_turned = q_total * q_cos + pltpu.roll(q_total, half, 1) * q_sin
    q_head = q_turned.astype(bf16).astype(f32)
    quarters = []
    for xx in range(nx):
        low = q_head if xx == 0 else pltpu.roll(q_head, HD - xx * quarter, 1)
        high = pltpu.roll(q_head, (HD - half - xx * quarter + quarter) % HD, 1)
        picked = jnp.where(lane < quarter, low, jnp.where(lane < half, high, 0.0))
        quarters.append(picked.astype(bf16))

    own_seg.wait()
    seg_wait = lambda plane, xx: remote(
        seg, seg_buf.at[plane, xx], s_seg.at[0], r_seg.at[plane, xx], here
    ).wait_recv()
    seg_wait(1, other)
    own_piece.wait()
    for pair in pairs[1:]:
        kv_wait(1, *pair)

    @pl.when(z > 0)
    def _():
        for xx in range(nx):
            seg_wait(0, xx)
        for pair in pairs:
            kv_wait(0, *pair)

    key_seg = jnp.concatenate(
        [seg_buf[plane, xx] for plane in range(2) for xx in range(nx)], axis=1
    )
    own_seg_row = key_seg[:, rows:]
    seg_column = jnp.transpose(jnp.broadcast_to(own_seg_row, (HD, rows)))[:, :1]
    key_pos = lax.broadcasted_iota(jnp.int32, (1, 2 * rows), 1) - rows
    keys = [
        jnp.concatenate([kv_all[0, xx], kv_all[1, xx]], axis=0) for xx in range(nx)
    ]
    step_rows = rows // nf
    for b in range(nf):
        span = slice(b * step_rows, (b + 1) * step_rows)
        query_pos = b * step_rows + lax.broadcasted_iota(jnp.int32, (step_rows, 1), 0)
        score = None
        for xx in range(nx):
            term = lax.dot_general(
                quarters[xx][span], keys[xx], (((1,), (1,)), ((), ())),
                preferred_element_type=f32,
            )
            score = term if score is None else score + term
        allowed = (key_pos <= query_pos) & (key_seg == seg_column[span])
        masked = jnp.where(allowed, score * HD ** (-0.5), NEG_FILL)
        row_max = jnp.max(masked, axis=1, keepdims=True)
        weight = jnp.where(allowed, jnp.exp(masked - row_max), 0.0)
        row_total = jnp.sum(weight, axis=1, keepdims=True)
        rounded = weight.astype(bf16)
        product = [
            jnp.dot(rounded, keys[xx], preferred_element_type=f32) for xx in range(nx)
        ]
        mixed = None
        for xx in reversed(range(nx)):
            low = pltpu.roll(product[xx], (half + xx * quarter) % HD, 1)
            high = pltpu.roll(product[xx], (HD - (nx - 1 - xx) * quarter) % HD, 1)
            lane_block = lane // quarter
            value = jnp.where(lane_block < nx, low, high)
            mixed = value if mixed is None else jnp.where(lane_block % nx == xx, value, mixed)
        mix_own[span, :] = (mixed / row_total).astype(bf16)

    wo_end(1)
    head = f * nx + x

    def mix_send(dx, d):
        ff, xx = lax.rem(f + d, nf), lax.rem(x + dx, nx)
        return remote(
            mix_own.at[tile(xx, tok)], mix_buf.at[:, tile(head, HD)],
            s_mix.at[dx, d], r_mix.at[x, f], dev(ff, z, xx),
        )

    def mix_wait(dx, d):
        ff, xx = lax.rem(f + d, nf), lax.rem(x + dx, nx)
        remote(
            mix_own.at[tile(x, tok)], mix_buf.at[:, tile(ff * nx + xx, HD)],
            s_mix.at[dx, d], r_mix.at[xx, ff], here,
        ).wait_recv()

    for pair in pairs[1:]:
        mix_send(*pair).start()
    own_mix = pltpu.make_async_copy(
        mix_own.at[tile(x, tok)], mix_buf.at[:, tile(head, HD)], s_loc.at[6]
    )
    own_mix.start()
    for d in range(2, nz):
        wo_end(d)
    own_mix.wait()
    own_wo.wait()
    for pair in pairs[1:]:
        mix_wait(*pair)
    for c in range(WO_CHUNKS):
        for j in range(nz):
            wo_wait(j, other, c)
        out[:, c * chunk : (c + 1) * chunk] = jnp.dot(
            mix_buf[...], wo_buf[:, c * chunk : (c + 1) * chunk], preferred_element_type=f32
        ).astype(bf16)

    hid_send.wait_send()
    seg_same.wait_send()
    for d in range(1, nz):
        wkv_send(d).wait_send()
    for d in range(1, nf):
        kvp_send(d).wait_send()
        q_send(lax.rem(f + d, nf)).wait_send()
    for pair in pairs[1:]:
        kv_send(1, *pair).wait_send()
        mix_send(*pair).wait_send()

    @pl.when(z < nz - 1)
    def _():
        for xx in range(nx):
            seg_next(xx).wait_send()
        for pair in pairs:
            kv_send(0, *pair).wait_send()

    for j in range(nz):
        for c in range(WO_CHUNKS):
            wo_cross(j, c).wait_send()

        @pl.when((z < nz - 1) & (z >= j))
        def _():
            wq_copy(wq, j, True).wait_send()
            for c in range(WO_CHUNKS):
                wo_copy(j, c, True).wait_send()

        @pl.when((z > 0) & (z <= j))
        def _():
            wq_copy(wq, j, False).wait_send()
            for c in range(WO_CHUNKS):
                wo_copy(j, c, False).wait_send()


def fused_on_device(nf, nz, nx, hidden, w_query, w_keyvalue, w_output, segment_ids):
    tok, kdim = hidden.shape
    cols = w_output.shape[1]
    rows = tok * nx
    sub = rows // nf
    kvw = w_keyvalue.shape[1]
    f32, bf16 = jnp.float32, jnp.bfloat16
    dma = pltpu.SemaphoreType.DMA
    vmem = pl.BlockSpec(memory_space=pltpu.VMEM)
    scratch = [
        pltpu.VMEM((rows, kdim), bf16),
        pltpu.VMEM((nz, kdim, HD), bf16),
        pltpu.VMEM((nz * kvw, kdim), bf16),
        pltpu.VMEM((nz * nx * HD, cols), bf16),
        pltpu.VMEM((2, nx, 1, tok), jnp.int32),
        pltpu.VMEM((nz, rows, HD), f32),
        pltpu.VMEM((nf, rows, HD), f32),
        pltpu.VMEM((rows, nz * kvw), f32),
        pltpu.VMEM((nf, sub, nz * kvw), f32),
        pltpu.VMEM((sub, HD), bf16),
        pltpu.VMEM((2, nx, rows, HD), bf16),
        pltpu.VMEM((rows, HD), bf16),
        pltpu.VMEM((tok, nz * nx * HD), bf16),
        dma((7,)), dma, dma, dma((1 + nx,)), dma((2, nx)),
        dma((nz,)), dma((nz,)), dma((nz,)), dma((nz,)), dma((nz,)),
        dma((nz,)), dma((nf,)), dma((nf,)), dma((nf,)),
        dma((2, nx, nf)), dma((2, nx, nf)),
        dma((nz, WO_CHUNKS)), dma((nz, WO_CHUNKS)), dma((nz, WO_CHUNKS)),
        dma((nz * nx, WO_CHUNKS)), dma((nx, nf)), dma((nx, nf)),
    ]
    return pl.pallas_call(
        functools.partial(fused_kernel, nf, nz, nx),
        out_shape=jax.ShapeDtypeStruct((tok, cols), bf16),
        in_specs=[vmem] * 5,
        out_specs=vmem,
        scratch_shapes=scratch,
        name="fused_sublayer",
        compiler_params=pltpu.CompilerParams(
            has_side_effects=True, vmem_limit_bytes=60 * 1024 * 1024
        ),
    )(hidden, w_query, w_keyvalue.T, w_output, segment_ids.reshape(1, tok))


def solution(mesh):
    in_specs = (P("sp", "fsdp"), P("fsdp", "sp"), P("fsdp", "sp"), P("sp", "fsdp"), P("sp"))
    out_specs = P("sp", "fsdp")
    nf, sp = mesh.shape["fsdp"], mesh.shape["sp"]
    if sp == GROUP and sp == 2 * nf:
        body = functools.partial(fused_on_device, nf, nf, sp // nf)
    else:
        body = on_device
    return jax.shard_map(
        body, mesh=mesh, in_specs=in_specs, out_specs=out_specs, check_vma=False
    )
```

```python
import functools
import math

import jax
import jax.numpy as jnp
from jax import lax
from jax.experimental import pallas as pl
from jax.experimental.pallas import tpu as pltpu
from jax.sharding import PartitionSpec as P

HD = 128
GROUP = 8


ROPE_BASE = 500000.0
NEG_FILL = -1e30


def rotate(values, positions, head_count, width):
    row_count = values.shape[0]
    shaped = values.reshape(row_count, head_count, width)
    half_width = width // 2
    frequency = jnp.exp(
        jnp.arange(half_width, dtype=jnp.float32) * (-2.0 * math.log(ROPE_BASE) / width)
    )
    angles = positions.astype(jnp.float32)[:, None] * frequency[None, :]
    cosine = jnp.cos(angles)[:, None, :]
    sine_part = jnp.sin(angles)[:, None, :]
    lower_half = shaped[:, :, :half_width]
    upper_half = shaped[:, :, half_width:]
    turned = jnp.concatenate(
        [
            lower_half * cosine - upper_half * sine_part,
            upper_half * cosine + lower_half * sine_part,
        ],
        axis=2,
    )
    return turned.reshape(row_count, head_count * width)


def split_keys(kv_sum, positions, kv_count, width):
    row_count = kv_sum.shape[0]
    shaped = kv_sum.reshape(row_count, kv_count, 2, width)
    key_part = rotate(
        shaped[:, :, 0, :].reshape(row_count, kv_count * width), positions, kv_count, width
    )
    key_part = key_part.reshape(row_count, kv_count, 1, width)
    return jnp.concatenate([key_part, shaped[:, :, 1:2, :]], axis=2).astype(jnp.bfloat16)


def merge_keys(
    state_in, query_tile, query_pos_tile, query_seg_tile, key_tile, key_pos_tile, key_seg_tile
):
    running_max, running_sum, weighted = state_in
    allowed = (key_pos_tile[None, :] <= query_pos_tile[:, None]) & (
        key_seg_tile[None, :] == query_seg_tile[:, None]
    )
    key_part = key_tile[:, :HD]
    value_part = key_tile[:, HD:]
    scores = lax.dot_general(
        query_tile, key_part, (((1,), (1,)), ((), ())), preferred_element_type=jnp.float32
    ) * HD ** (-0.5)
    masked = jnp.where(allowed, scores, NEG_FILL)
    new_max = jnp.maximum(running_max, jnp.max(masked, axis=1))
    weights = jnp.where(allowed, jnp.exp(masked - new_max[:, None]), 0.0)
    new_sum = jnp.sum(weights, axis=1)
    new_weighted = jnp.dot(
        weights.astype(jnp.bfloat16), value_part, preferred_element_type=jnp.float32
    )
    return (new_max, new_sum, new_weighted)


def on_device(hidden, w_query, w_keyvalue, w_output, segment_ids):
    fsdp_count = lax.axis_size("fsdp")
    seq_count = lax.axis_size("sp")
    fsdp_index = lax.axis_index("fsdp")
    seq_index = lax.axis_index("sp")
    tok_rows = hidden.shape[0]
    sub_rows = tok_rows // fsdp_count
    kv_count = seq_count // GROUP
    query_rows = seq_count * sub_rows
    offsets = jnp.arange(query_rows, dtype=jnp.int32)
    query_pos = offsets // sub_rows * tok_rows + fsdp_index * sub_rows + offsets % sub_rows
    own_positions = (
        seq_index * tok_rows + fsdp_index * sub_rows + jnp.arange(sub_rows, dtype=jnp.int32)
    )

    def project(weight_block):
        return jnp.dot(hidden, weight_block, preferred_element_type=jnp.float32)

    query_part = project(lax.all_gather(w_query, "sp", axis=1, tiled=True))
    kv_part = project(lax.all_gather(w_keyvalue, "sp", axis=1, tiled=True))
    query_sum, kv_sum = (
        lax.psum_scatter(query_part, "fsdp", scatter_dimension=0, tiled=True),
        lax.psum_scatter(kv_part, "fsdp", scatter_dimension=0, tiled=True),
    )
    query_local = rotate(query_sum, own_positions, seq_count, HD).astype(jnp.bfloat16)
    pairs = split_keys(kv_sum, own_positions, kv_count, HD)
    expanded = jnp.repeat(pairs, GROUP, axis=1).reshape(sub_rows, seq_count * 2 * HD)
    query_head, kv_head = (
        lax.all_to_all(query_local, "sp", split_axis=1, concat_axis=0, tiled=True),
        lax.all_to_all(expanded, "sp", split_axis=1, concat_axis=0, tiled=True),
    )
    segment_all = lax.all_gather(segment_ids, "sp", axis=0, tiled=True)
    query_seg = segment_all[query_pos]
    initial = (
        jnp.full((query_rows,), NEG_FILL, jnp.float32),
        jnp.zeros((query_rows,), jnp.float32),
        jnp.zeros((query_rows, HD), jnp.float32),
    )
    block_keys = lax.all_gather(kv_head, "fsdp", axis=0, tiled=True)
    piece_rows = block_keys.shape[0]
    row_ids = jnp.arange(piece_rows, dtype=jnp.int32)
    source_id = row_ids // query_rows
    within = row_ids % query_rows
    key_pos = within // sub_rows * tok_rows + source_id * sub_rows + within % sub_rows
    key_seg = segment_all[key_pos]
    final_max, final_sum, final_weighted = merge_keys(
        initial, query_head, query_pos, query_seg, block_keys, key_pos, key_seg
    )
    attention = (final_weighted / final_sum[:, None]).astype(jnp.bfloat16)
    back_rows = lax.all_to_all(attention, "sp", split_axis=0, concat_axis=1, tiled=True)
    mixed_rows = lax.all_gather(back_rows, "fsdp", axis=0, tiled=True)
    result = jnp.dot(
        mixed_rows,
        lax.all_gather(w_output, "sp", axis=0, tiled=True),
        preferred_element_type=jnp.float32,
    )
    return result.astype(jnp.bfloat16)


NEG_POS = -1
WO_CHUNKS = 4


def fused_kernel(
    nf, nz, nx, hid, wq, wkv, wo, seg, out,
    h_buf, wq_buf, wkv_buf, wo_buf, seg_buf,
    q_part, q_recv, kv_part, kv_recv, kv_piece, kv_all, mix_own, mix_buf,
    s_loc, s_hid, r_hid, s_seg, r_seg, s_wkv, r_wkv, s_wqr, s_wql, r_wq,
    s_q, r_q, s_kvp, r_kvp, s_kv, r_kv, s_wor, s_wol, s_wox, r_wo, s_mix, r_mix,
):
    f = lax.axis_index("fsdp")
    s = lax.axis_index("sp")
    z, x = s // nx, s % nx
    tok, kdim = hid.shape
    rows = tok * nx
    sub = rows // nf
    kvw = wkv.shape[0]
    other = 1 - x
    chunk = wo.shape[1] // WO_CHUNKS
    f32, bf16 = jnp.float32, jnp.bfloat16

    def dev(ff, zz, xx):
        return (ff, zz * nx + xx)

    def remote(src, dst, ss, rs, target):
        return pltpu.make_async_remote_copy(
            src_ref=src, dst_ref=dst, send_sem=ss, recv_sem=rs,
            device_id=target, device_id_type=pl.DeviceIdType.MESH,
        )

    def tile(ref, count):
        return pl.ds(pl.multiple_of(ref * count, count), count)

    here = (f, s)
    own_h = pltpu.make_async_copy(hid, h_buf.at[tile(x, tok)], s_loc.at[0])
    own_wq = pltpu.make_async_copy(wq, wq_buf.at[z], s_loc.at[1])
    own_wkv = pltpu.make_async_copy(wkv, wkv_buf.at[tile(z, kvw)], s_loc.at[2])
    own_wo = pltpu.make_async_copy(wo, wo_buf.at[tile(s, HD)], s_loc.at[3])
    own_seg = pltpu.make_async_copy(seg, seg_buf.at[1, x], s_loc.at[4])
    hid_send = remote(hid, h_buf.at[tile(x, tok)], s_hid, r_hid, dev(f, z, other))

    def hid_wait():
        remote(hid, h_buf.at[tile(other, tok)], s_hid, r_hid, here).wait_recv()

    def wkv_send(d):
        zz = lax.rem(z + d, nz)
        return remote(
            wkv, wkv_buf.at[tile(z, kvw)], s_wkv.at[d - 1], r_wkv.at[z], dev(f, zz, x)
        )

    def wkv_wait(d):
        zz = lax.rem(z + d, nz)
        remote(
            wkv, wkv_buf.at[tile(zz, kvw)], s_wkv.at[d - 1], r_wkv.at[zz], here
        ).wait_recv()

    def wq_copy(src, j, to_right):
        sems = s_wqr if to_right else s_wql
        return remote(
            src, wq_buf.at[j], sems.at[j], r_wq.at[j],
            dev(f, z + 1 if to_right else z - 1, x),
        )

    def wo_slice(zz, xx, c):
        return wo_buf.at[tile(zz * nx + xx, HD), c * chunk : (c + 1) * chunk]

    def wo_src(j, c, own):
        return wo.at[:, c * chunk : (c + 1) * chunk] if own else wo_slice(j, x, c)

    def wo_copy(j, c, to_right, own=False):
        sems = s_wor if to_right else s_wol
        return remote(
            wo_src(j, c, own), wo_slice(j, x, c), sems.at[j, c], r_wo.at[j * nx + x, c],
            dev(f, z + 1 if to_right else z - 1, x),
        )

    def wo_cross(j, c, own=False):
        return remote(
            wo_src(j, c, own), wo_slice(j, x, c), s_wox.at[j, c], r_wo.at[j * nx + x, c],
            dev(f, z, other),
        )

    def wo_wait(j, xx, c):
        remote(
            wo_slice(j, xx, c), wo_slice(j, xx, c), s_wox.at[j, c], r_wo.at[j * nx + xx, c], here
        ).wait_recv()

    def wo_own(to_right):
        for c in range(WO_CHUNKS):
            wo_copy(z, c, to_right, own=True).start()

    seg_same = remote(seg, seg_buf.at[1, x], s_seg.at[0], r_seg.at[1, x], dev(f, z, other))

    def seg_next(xx):
        return remote(
            seg, seg_buf.at[0, x], s_seg.at[1 + xx], r_seg.at[0, x], dev(f, z + 1, xx)
        )

    barrier = pltpu.get_barrier_semaphore()

    def greet(ff, zz, xx):
        pl.semaphore_signal(
            barrier, inc=1, device_id=dev(ff, zz, xx), device_id_type=pl.DeviceIdType.MESH
        )

    plane = nf * nx
    for step in (1, -1):
        @pl.when((z + step >= 0) & (z + step < nz))
        def _():
            for xx in range(nx):
                for ff in range(nf):
                    greet(ff, z + step, xx)

        for far in range(2, nz):
            @pl.when((z + far * step >= 0) & (z + far * step < nz))
            def _():
                greet(f, z + far * step, x)

    for d in range(1, plane):
        greet(lax.rem(f + d, nf), z, lax.rem(x + d // nf, nx))
    ends = jnp.where(z == 0, 1, 0) + jnp.where(z == nz - 1, 1, 0)
    pl.semaphore_wait(barrier, (3 - ends) * plane - 1 + nz - 3 + ends)

    for d in range(1, nz):
        wkv_send(d).start()

    @pl.when(z < nz - 1)
    def _():
        wq_copy(wq, z, True).start()

    @pl.when(z > 0)
    def _():
        wq_copy(wq, z, False).start()

    hid_send.start()
    seg_same.start()

    @pl.when(z < nz - 1)
    def _():
        for xx in range(nx):
            seg_next(xx).start()

    for copy in (own_h, own_wq, own_wkv, own_wo, own_seg):
        copy.start()

    @pl.when(z == 0)
    def _():
        wo_own(True)
        kv_all[0] = jnp.zeros(kv_all.shape[1:], bf16)
        seg_buf[0] = jnp.full(seg_buf.shape[1:], NEG_POS, jnp.int32)

    @pl.when(z == nz - 1)
    def _():
        wo_own(False)

    def table(row_count, first, lane_index):
        position = (first + lax.broadcasted_iota(jnp.int32, (row_count, HD), 0)).astype(f32)
        frequency = jnp.exp(lane_index.astype(f32) * (-2.0 * math.log(ROPE_BASE) / HD))
        return position * frequency

    lane = lax.broadcasted_iota(jnp.int32, (1, HD), 1)
    half = HD // 2
    quarter = half // nx
    kv_angle = table(sub, z * rows + f * sub, x * quarter + lane % quarter)
    is_key = lane < half
    kv_cos = jnp.where(is_key, jnp.cos(kv_angle), 1.0)
    kv_sin = jnp.where(is_key, jnp.sin(kv_angle), 0.0)
    kv_sin = jnp.where(lane < quarter, -kv_sin, kv_sin)

    def wq_step(d):
        @pl.when(z >= d)
        def _():
            j = z - d
            wq_copy(wq_buf.at[j], j, True).wait_recv()

            @pl.when(z < nz - 1)
            def _():
                wq_copy(wq_buf.at[j], j, True).start()

                @pl.when(z == d)
                def _():
                    wo_own(True)

        @pl.when(z + d < nz)
        def _():
            j = z + d
            wq_copy(wq_buf.at[j], j, False).wait_recv()

            @pl.when(z > 0)
            def _():
                wq_copy(wq_buf.at[j], j, False).start()

                @pl.when(z + d == nz - 1)
                def _():
                    wo_own(False)

    def q_send(j):
        return remote(q_part.at[j], q_recv.at[f], s_q.at[j], r_q.at[f], (j, s))

    def q_project(j):
        q_part[j] = jnp.dot(h_buf[...], wq_buf[j], preferred_element_type=f32)

        @pl.when(j != f)
        def _():
            q_send(j).start()

    def q_step(d):
        @pl.when(z >= d)
        def _():
            q_project(z - d)

        @pl.when(z + d < nz)
        def _():
            q_project(z + d)

    wq_step(1)
    own_h.wait()
    own_wq.wait()
    own_wkv.wait()
    hid_wait()
    for c in range(WO_CHUNKS):
        wo_cross(z, c, own=True).start()
    for d in range(1, nz):
        wkv_wait(d)
    kv_part[...] = lax.dot_general(
        h_buf[...], wkv_buf[...], (((1,), (1,)), ((), ())), preferred_element_type=f32
    )

    def kvp_send(d):
        ff = lax.rem(f + d, nf)
        return remote(
            kv_part.at[tile(ff, sub)], kv_recv.at[f], s_kvp.at[d - 1], r_kvp.at[f], (ff, s)
        )

    def kvp_wait(d):
        ff = lax.rem(f + d, nf)
        remote(
            kv_part.at[tile(ff, sub)], kv_recv.at[ff], s_kvp.at[d - 1], r_kvp.at[ff], here
        ).wait_recv()

    for d in range(1, nf):
        kvp_send(d).start()
    if nz > 2:
        wq_step(2)
    q_project(z)
    q_step(1)
    total = kv_part[tile(f, sub), :]
    for d in range(1, nf):
        kvp_wait(d)
        total = total + kv_recv[lax.rem(f + d, nf)]
    partner = jnp.where(
        lane < quarter, pltpu.roll(total, HD - quarter, 1), pltpu.roll(total, quarter, 1)
    )
    kv_piece[...] = (total * kv_cos + partner * kv_sin).astype(bf16)
    piece_rows = tile(f, sub)
    own_piece = pltpu.make_async_copy(kv_piece, kv_all.at[1, x, piece_rows], s_loc.at[5])
    own_piece.start()

    def kv_send(plane, dx, d):
        ff, xx = lax.rem(f + d, nf), lax.rem(x + dx, nx)
        return remote(
            kv_piece, kv_all.at[plane, x, piece_rows],
            s_kv.at[plane, dx, d], r_kv.at[plane, x, f], dev(ff, z + 1 - plane, xx),
        )

    def kv_wait(plane, dx, d):
        ff, xx = lax.rem(f + d, nf), lax.rem(x + dx, nx)
        remote(
            kv_piece, kv_all.at[plane, xx, tile(ff, sub)],
            s_kv.at[plane, dx, d], r_kv.at[plane, xx, ff], here,
        ).wait_recv()

    pairs = [(dx, d) for dx in range(nx) for d in range(nf)]
    for pair in pairs[1:]:
        kv_send(1, *pair).start()

    @pl.when(z < nz - 1)
    def _():
        for pair in pairs:
            kv_send(0, *pair).start()

    for d in range(2, nz):
        if d > 2:
            wq_step(d)
        q_step(d)

    def wo_side(j, to_right):
        for c in range(WO_CHUNKS):
            wo_wait(j, x, c)
            if to_right is not None:
                wo_copy(j, c, to_right).start()
            wo_cross(j, c).start()

    def wo_mid(d):
        @pl.when((z >= d) & (z < nz - 1))
        def _():
            wo_side(z - d, True)

        @pl.when((z + d < nz) & (z > 0))
        def _():
            wo_side(z + d, False)

    def wo_end(d):
        if d < nz:
            @pl.when((z >= d) & (z == nz - 1))
            def _():
                wo_side(z - d, None)

            @pl.when((z + d < nz) & (z == 0))
            def _():
                wo_side(z + d, None)

    for d in range(1, nz - 1):
        wo_mid(d)

    q_angle = table(rows, z * rows, lane % half)
    q_cos = jnp.cos(q_angle)
    q_sin = jnp.where(lane < half, -jnp.sin(q_angle), jnp.sin(q_angle))
    q_total = q_part[f]
    for d in range(1, nf):
        ff = lax.rem(f + d, nf)
        remote(q_part.at[0], q_recv.at[ff], s_q.at[0], r_q.at[ff], here).wait_recv()
        q_total = q_total + q_recv[ff]
    q_turned = q_total * q_cos + pltpu.roll(q_total, half, 1) * q_sin
    q_head = q_turned.astype(bf16).astype(f32)
    quarters = []
    for xx in range(nx):
        low = q_head if xx == 0 else pltpu.roll(q_head, HD - xx * quarter, 1)
        high = pltpu.roll(q_head, (HD - half - xx * quarter + quarter) % HD, 1)
        picked = jnp.where(lane < quarter, low, jnp.where(lane < half, high, 0.0))
        quarters.append(picked.astype(bf16))

    own_seg.wait()
    seg_wait = lambda plane, xx: remote(
        seg, seg_buf.at[plane, xx], s_seg.at[0], r_seg.at[plane, xx], here
    ).wait_recv()
    seg_wait(1, other)
    own_piece.wait()
    for pair in pairs[1:]:
        kv_wait(1, *pair)

    @pl.when(z > 0)
    def _():
        for xx in range(nx):
            seg_wait(0, xx)
        for pair in pairs:
            kv_wait(0, *pair)

    key_seg = jnp.concatenate(
        [seg_buf[plane, xx] for plane in range(2) for xx in range(nx)], axis=1
    )
    own_seg_row = key_seg[:, rows:]
    seg_column = jnp.transpose(jnp.broadcast_to(own_seg_row, (HD, rows)))[:, :1]
    key_pos = lax.broadcasted_iota(jnp.int32, (1, 2 * rows), 1) - rows
    keys = [
        jnp.concatenate([kv_all[0, xx], kv_all[1, xx]], axis=0) for xx in range(nx)
    ]
    step_rows = rows // nf
    for b in range(nf):
        span = slice(b * step_rows, (b + 1) * step_rows)
        query_pos = b * step_rows + lax.broadcasted_iota(jnp.int32, (step_rows, 1), 0)
        score = None
        for xx in range(nx):
            term = lax.dot_general(
                quarters[xx][span], keys[xx], (((1,), (1,)), ((), ())),
                preferred_element_type=f32,
            )
            score = term if score is None else score + term
        allowed = (key_pos <= query_pos) & (key_seg == seg_column[span])
        masked = jnp.where(allowed, score * HD ** (-0.5), NEG_FILL)
        row_max = jnp.max(masked, axis=1, keepdims=True)
        weight = jnp.where(allowed, jnp.exp(masked - row_max), 0.0)
        row_total = jnp.sum(weight, axis=1, keepdims=True)
        rounded = weight.astype(bf16)
        product = [
            jnp.dot(rounded, keys[xx], preferred_element_type=f32) for xx in range(nx)
        ]
        mixed = None
        for xx in reversed(range(nx)):
            low = pltpu.roll(product[xx], (half + xx * quarter) % HD, 1)
            high = pltpu.roll(product[xx], (HD - (nx - 1 - xx) * quarter) % HD, 1)
            lane_block = lane // quarter
            value = jnp.where(lane_block < nx, low, high)
            mixed = value if mixed is None else jnp.where(lane_block % nx == xx, value, mixed)
        mix_own[span, :] = (mixed / row_total).astype(bf16)

    head = f * nx + x

    def mix_send(dx, d):
        ff, xx = lax.rem(f + d, nf), lax.rem(x + dx, nx)
        return remote(
            mix_own.at[tile(xx, tok)], mix_buf.at[:, tile(head, HD)],
            s_mix.at[dx, d], r_mix.at[x, f], dev(ff, z, xx),
        )

    def mix_wait(dx, d):
        ff, xx = lax.rem(f + d, nf), lax.rem(x + dx, nx)
        remote(
            mix_own.at[tile(x, tok)], mix_buf.at[:, tile(ff * nx + xx, HD)],
            s_mix.at[dx, d], r_mix.at[xx, ff], here,
        ).wait_recv()

    for pair in pairs[1:]:
        mix_send(*pair).start()
    own_mix = pltpu.make_async_copy(
        mix_own.at[tile(x, tok)], mix_buf.at[:, tile(head, HD)], s_loc.at[6]
    )
    own_mix.start()
    for d in range(1, nz - 1):
        wo_end(d)
    own_mix.wait()
    own_wo.wait()
    for pair in pairs[1:]:
        mix_wait(*pair)

    def wo_last(c):
        for end, j in ((0, nz - 1), (nz - 1, 0)):
            @pl.when(z == end)
            def _():
                wo_wait(j, x, c)
                wo_cross(j, c).start()

    wo_last(0)
    for c in range(WO_CHUNKS):
        if c + 1 < WO_CHUNKS:
            wo_last(c + 1)
        for j in range(nz):
            wo_wait(j, other, c)
        out[:, c * chunk : (c + 1) * chunk] = jnp.dot(
            mix_buf[...], wo_buf[:, c * chunk : (c + 1) * chunk], preferred_element_type=f32
        ).astype(bf16)

    hid_send.wait_send()
    seg_same.wait_send()
    for d in range(1, nz):
        wkv_send(d).wait_send()
    for d in range(1, nf):
        kvp_send(d).wait_send()
        q_send(lax.rem(f + d, nf)).wait_send()
    for pair in pairs[1:]:
        kv_send(1, *pair).wait_send()
        mix_send(*pair).wait_send()

    @pl.when(z < nz - 1)
    def _():
        for xx in range(nx):
            seg_next(xx).wait_send()
        for pair in pairs:
            kv_send(0, *pair).wait_send()

    for j in range(nz):
        for c in range(WO_CHUNKS):
            wo_cross(j, c).wait_send()

        @pl.when((z < nz - 1) & (z >= j))
        def _():
            wq_copy(wq, j, True).wait_send()
            for c in range(WO_CHUNKS):
                wo_copy(j, c, True).wait_send()

        @pl.when((z > 0) & (z <= j))
        def _():
            wq_copy(wq, j, False).wait_send()
            for c in range(WO_CHUNKS):
                wo_copy(j, c, False).wait_send()


def fused_on_device(nf, nz, nx, hidden, w_query, w_keyvalue, w_output, segment_ids):
    tok, kdim = hidden.shape
    cols = w_output.shape[1]
    rows = tok * nx
    sub = rows // nf
    kvw = w_keyvalue.shape[1]
    f32, bf16 = jnp.float32, jnp.bfloat16
    dma = pltpu.SemaphoreType.DMA
    vmem = pl.BlockSpec(memory_space=pltpu.VMEM)
    scratch = [
        pltpu.VMEM((rows, kdim), bf16),
        pltpu.VMEM((nz, kdim, HD), bf16),
        pltpu.VMEM((nz * kvw, kdim), bf16),
        pltpu.VMEM((nz * nx * HD, cols), bf16),
        pltpu.VMEM((2, nx, 1, tok), jnp.int32),
        pltpu.VMEM((nz, rows, HD), f32),
        pltpu.VMEM((nf, rows, HD), f32),
        pltpu.VMEM((rows, nz * kvw), f32),
        pltpu.VMEM((nf, sub, nz * kvw), f32),
        pltpu.VMEM((sub, HD), bf16),
        pltpu.VMEM((2, nx, rows, HD), bf16),
        pltpu.VMEM((rows, HD), bf16),
        pltpu.VMEM((tok, nz * nx * HD), bf16),
        dma((7,)), dma, dma, dma((1 + nx,)), dma((2, nx)),
        dma((nz,)), dma((nz,)), dma((nz,)), dma((nz,)), dma((nz,)),
        dma((nz,)), dma((nf,)), dma((nf,)), dma((nf,)),
        dma((2, nx, nf)), dma((2, nx, nf)),
        dma((nz, WO_CHUNKS)), dma((nz, WO_CHUNKS)), dma((nz, WO_CHUNKS)),
        dma((nz * nx, WO_CHUNKS)), dma((nx, nf)), dma((nx, nf)),
    ]
    return pl.pallas_call(
        functools.partial(fused_kernel, nf, nz, nx),
        out_shape=jax.ShapeDtypeStruct((tok, cols), bf16),
        in_specs=[vmem] * 5,
        out_specs=vmem,
        scratch_shapes=scratch,
        name="fused_sublayer",
        compiler_params=pltpu.CompilerParams(
            collective_id=0, has_side_effects=True, vmem_limit_bytes=60 * 1024 * 1024
        ),
    )(hidden, w_query, w_keyvalue.T, w_output, segment_ids.reshape(1, tok))


def solution(mesh):
    in_specs = (P("sp", "fsdp"), P("fsdp", "sp"), P("fsdp", "sp"), P("sp", "fsdp"), P("sp"))
    out_specs = P("sp", "fsdp")
    nf, sp = mesh.shape["fsdp"], mesh.shape["sp"]
    if sp == GROUP and sp == 2 * nf:
        body = functools.partial(fused_on_device, nf, nf, sp // nf)
    else:
        body = on_device
    return jax.shard_map(
        body, mesh=mesh, in_specs=in_specs, out_specs=out_specs, check_vma=False
    )
```

```python
import functools
import math

import jax
import jax.numpy as jnp
from jax import lax
from jax.experimental import pallas as pl
from jax.experimental.pallas import tpu as pltpu
from jax.sharding import PartitionSpec as P

HD = 128
GROUP = 8


ROPE_BASE = 500000.0
NEG_FILL = -1e30


def rotate(values, positions, head_count, width):
    row_count = values.shape[0]
    shaped = values.reshape(row_count, head_count, width)
    half_width = width // 2
    frequency = jnp.exp(
        jnp.arange(half_width, dtype=jnp.float32) * (-2.0 * math.log(ROPE_BASE) / width)
    )
    angles = positions.astype(jnp.float32)[:, None] * frequency[None, :]
    cosine = jnp.cos(angles)[:, None, :]
    sine_part = jnp.sin(angles)[:, None, :]
    lower_half = shaped[:, :, :half_width]
    upper_half = shaped[:, :, half_width:]
    turned = jnp.concatenate(
        [
            lower_half * cosine - upper_half * sine_part,
            upper_half * cosine + lower_half * sine_part,
        ],
        axis=2,
    )
    return turned.reshape(row_count, head_count * width)


def split_keys(kv_sum, positions, kv_count, width):
    row_count = kv_sum.shape[0]
    shaped = kv_sum.reshape(row_count, kv_count, 2, width)
    key_part = rotate(
        shaped[:, :, 0, :].reshape(row_count, kv_count * width), positions, kv_count, width
    )
    key_part = key_part.reshape(row_count, kv_count, 1, width)
    return jnp.concatenate([key_part, shaped[:, :, 1:2, :]], axis=2).astype(jnp.bfloat16)


def merge_keys(
    state_in, query_tile, query_pos_tile, query_seg_tile, key_tile, key_pos_tile, key_seg_tile
):
    running_max, running_sum, weighted = state_in
    allowed = (key_pos_tile[None, :] <= query_pos_tile[:, None]) & (
        key_seg_tile[None, :] == query_seg_tile[:, None]
    )
    key_part = key_tile[:, :HD]
    value_part = key_tile[:, HD:]
    scores = lax.dot_general(
        query_tile, key_part, (((1,), (1,)), ((), ())), preferred_element_type=jnp.float32
    ) * HD ** (-0.5)
    masked = jnp.where(allowed, scores, NEG_FILL)
    new_max = jnp.maximum(running_max, jnp.max(masked, axis=1))
    weights = jnp.where(allowed, jnp.exp(masked - new_max[:, None]), 0.0)
    new_sum = jnp.sum(weights, axis=1)
    new_weighted = jnp.dot(
        weights.astype(jnp.bfloat16), value_part, preferred_element_type=jnp.float32
    )
    return (new_max, new_sum, new_weighted)


def on_device(hidden, w_query, w_keyvalue, w_output, segment_ids):
    fsdp_count = lax.axis_size("fsdp")
    seq_count = lax.axis_size("sp")
    fsdp_index = lax.axis_index("fsdp")
    seq_index = lax.axis_index("sp")
    tok_rows = hidden.shape[0]
    sub_rows = tok_rows // fsdp_count
    kv_count = seq_count // GROUP
    query_rows = seq_count * sub_rows
    offsets = jnp.arange(query_rows, dtype=jnp.int32)
    query_pos = offsets // sub_rows * tok_rows + fsdp_index * sub_rows + offsets % sub_rows
    own_positions = (
        seq_index * tok_rows + fsdp_index * sub_rows + jnp.arange(sub_rows, dtype=jnp.int32)
    )

    def project(weight_block):
        return jnp.dot(hidden, weight_block, preferred_element_type=jnp.float32)

    query_part = project(lax.all_gather(w_query, "sp", axis=1, tiled=True))
    kv_part = project(lax.all_gather(w_keyvalue, "sp", axis=1, tiled=True))
    query_sum, kv_sum = (
        lax.psum_scatter(query_part, "fsdp", scatter_dimension=0, tiled=True),
        lax.psum_scatter(kv_part, "fsdp", scatter_dimension=0, tiled=True),
    )
    query_local = rotate(query_sum, own_positions, seq_count, HD).astype(jnp.bfloat16)
    pairs = split_keys(kv_sum, own_positions, kv_count, HD)
    expanded = jnp.repeat(pairs, GROUP, axis=1).reshape(sub_rows, seq_count * 2 * HD)
    query_head, kv_head = (
        lax.all_to_all(query_local, "sp", split_axis=1, concat_axis=0, tiled=True),
        lax.all_to_all(expanded, "sp", split_axis=1, concat_axis=0, tiled=True),
    )
    segment_all = lax.all_gather(segment_ids, "sp", axis=0, tiled=True)
    query_seg = segment_all[query_pos]
    initial = (
        jnp.full((query_rows,), NEG_FILL, jnp.float32),
        jnp.zeros((query_rows,), jnp.float32),
        jnp.zeros((query_rows, HD), jnp.float32),
    )
    block_keys = lax.all_gather(kv_head, "fsdp", axis=0, tiled=True)
    piece_rows = block_keys.shape[0]
    row_ids = jnp.arange(piece_rows, dtype=jnp.int32)
    source_id = row_ids // query_rows
    within = row_ids % query_rows
    key_pos = within // sub_rows * tok_rows + source_id * sub_rows + within % sub_rows
    key_seg = segment_all[key_pos]
    final_max, final_sum, final_weighted = merge_keys(
        initial, query_head, query_pos, query_seg, block_keys, key_pos, key_seg
    )
    attention = (final_weighted / final_sum[:, None]).astype(jnp.bfloat16)
    back_rows = lax.all_to_all(attention, "sp", split_axis=0, concat_axis=1, tiled=True)
    mixed_rows = lax.all_gather(back_rows, "fsdp", axis=0, tiled=True)
    result = jnp.dot(
        mixed_rows,
        lax.all_gather(w_output, "sp", axis=0, tiled=True),
        preferred_element_type=jnp.float32,
    )
    return result.astype(jnp.bfloat16)


NEG_POS = -1
WO_CHUNKS = 4


def fused_kernel(
    nf, nz, nx, hid, wq, wkv, wo, seg, out,
    h_buf, wq_buf, wkv_buf, wo_buf, seg_buf,
    q_part, q_recv, kv_part, kv_recv, kv_piece, kv_all, mix_own, mix_buf, q_cos, q_sin,
    s_loc, s_hid, r_hid, s_seg, r_seg, s_wkv, r_wkv, s_wqr, s_wql, r_wq,
    s_q, r_q, s_kvp, r_kvp, s_kv, r_kv, s_wor, s_wol, s_wox, r_wo, s_mix, r_mix,
):
    f = lax.axis_index("fsdp")
    s = lax.axis_index("sp")
    z, x = s // nx, s % nx
    tok, kdim = hid.shape
    rows = tok * nx
    sub = rows // nf
    kvw = wkv.shape[0]
    other = 1 - x
    chunk = wo.shape[1] // WO_CHUNKS
    f32, bf16 = jnp.float32, jnp.bfloat16

    def dev(ff, zz, xx):
        return (ff, zz * nx + xx)

    def remote(src, dst, ss, rs, target):
        return pltpu.make_async_remote_copy(
            src_ref=src, dst_ref=dst, send_sem=ss, recv_sem=rs,
            device_id=target, device_id_type=pl.DeviceIdType.MESH,
        )

    def tile(ref, count):
        return pl.ds(pl.multiple_of(ref * count, count), count)

    here = (f, s)
    own_h = pltpu.make_async_copy(hid, h_buf.at[tile(x, tok)], s_loc.at[0])
    own_wq = pltpu.make_async_copy(wq, wq_buf.at[z], s_loc.at[1])
    own_wkv = pltpu.make_async_copy(wkv, wkv_buf.at[tile(z, kvw)], s_loc.at[2])
    own_wo = pltpu.make_async_copy(wo, wo_buf.at[tile(s, HD)], s_loc.at[3])
    own_seg = pltpu.make_async_copy(seg, seg_buf.at[1, x], s_loc.at[4])
    hid_send = remote(hid, h_buf.at[tile(x, tok)], s_hid, r_hid, dev(f, z, other))

    def hid_wait():
        remote(hid, h_buf.at[tile(other, tok)], s_hid, r_hid, here).wait_recv()

    def wkv_send(d):
        zz = lax.rem(z + d, nz)
        return remote(
            wkv, wkv_buf.at[tile(z, kvw)], s_wkv.at[d - 1], r_wkv.at[z], dev(f, zz, x)
        )

    def wkv_wait(d):
        zz = lax.rem(z + d, nz)
        remote(
            wkv, wkv_buf.at[tile(zz, kvw)], s_wkv.at[d - 1], r_wkv.at[zz], here
        ).wait_recv()

    def wq_copy(src, j, to_right):
        sems = s_wqr if to_right else s_wql
        return remote(
            src, wq_buf.at[j], sems.at[j], r_wq.at[j],
            dev(f, z + 1 if to_right else z - 1, x),
        )

    def wo_slice(zz, xx, c):
        return wo_buf.at[tile(zz * nx + xx, HD), c * chunk : (c + 1) * chunk]

    def wo_src(j, c, own):
        return wo.at[:, c * chunk : (c + 1) * chunk] if own else wo_slice(j, x, c)

    def wo_copy(j, c, to_right, own=False):
        sems = s_wor if to_right else s_wol
        return remote(
            wo_src(j, c, own), wo_slice(j, x, c), sems.at[j, c], r_wo.at[j * nx + x, c],
            dev(f, z + 1 if to_right else z - 1, x),
        )

    def wo_cross(j, c, own=False):
        return remote(
            wo_src(j, c, own), wo_slice(j, x, c), s_wox.at[j, c], r_wo.at[j * nx + x, c],
            dev(f, z, other),
        )

    def wo_wait(j, xx, c):
        remote(
            wo_slice(j, xx, c), wo_slice(j, xx, c), s_wox.at[j, c], r_wo.at[j * nx + xx, c], here
        ).wait_recv()

    def wo_own(to_right):
        for c in range(WO_CHUNKS):
            wo_copy(z, c, to_right, own=True).start()

    seg_same = remote(seg, seg_buf.at[1, x], s_seg.at[0], r_seg.at[1, x], dev(f, z, other))

    def seg_next(xx):
        return remote(
            seg, seg_buf.at[0, x], s_seg.at[1 + xx], r_seg.at[0, x], dev(f, z + 1, xx)
        )

    barrier = pltpu.get_barrier_semaphore()

    def greet(ff, zz, xx):
        pl.semaphore_signal(
            barrier, inc=1, device_id=dev(ff, zz, xx), device_id_type=pl.DeviceIdType.MESH
        )

    plane = nf * nx
    for step in (1, -1):
        @pl.when((z + step >= 0) & (z + step < nz))
        def _():
            for xx in range(nx):
                for ff in range(nf):
                    greet(ff, z + step, xx)

        for far in range(2, nz):
            @pl.when((z + far * step >= 0) & (z + far * step < nz))
            def _():
                greet(f, z + far * step, x)

    for d in range(1, plane):
        greet(lax.rem(f + d, nf), z, lax.rem(x + d // nf, nx))
    ends = jnp.where(z == 0, 1, 0) + jnp.where(z == nz - 1, 1, 0)
    pl.semaphore_wait(barrier, (3 - ends) * plane - 1 + nz - 3 + ends)

    for d in range(1, nz):
        wkv_send(d).start()

    @pl.when(z < nz - 1)
    def _():
        wq_copy(wq, z, True).start()

    @pl.when(z > 0)
    def _():
        wq_copy(wq, z, False).start()

    hid_send.start()
    seg_same.start()

    @pl.when(z < nz - 1)
    def _():
        for xx in range(nx):
            seg_next(xx).start()

    for copy in (own_h, own_wq, own_wkv, own_wo, own_seg):
        copy.start()

    @pl.when(z == 0)
    def _():
        wo_own(True)
        kv_all[0] = jnp.zeros(kv_all.shape[1:], bf16)
        seg_buf[0] = jnp.full(seg_buf.shape[1:], NEG_POS, jnp.int32)

    @pl.when(z == nz - 1)
    def _():
        wo_own(False)

    def table(row_count, first, lane_index):
        position = (first + lax.broadcasted_iota(jnp.int32, (row_count, HD), 0)).astype(f32)
        frequency = jnp.exp(lane_index.astype(f32) * (-2.0 * math.log(ROPE_BASE) / HD))
        return position * frequency

    lane = lax.broadcasted_iota(jnp.int32, (1, HD), 1)
    half = HD // 2
    quarter = half // nx
    kv_angle = table(sub, z * rows + f * sub, x * quarter + lane % quarter)
    is_key = lane < half
    kv_cos = jnp.where(is_key, jnp.cos(kv_angle), 1.0)
    kv_sin = jnp.where(is_key, jnp.sin(kv_angle), 0.0)
    kv_sin = jnp.where(lane < quarter, -kv_sin, kv_sin)
    q_angle = table(rows, z * rows, lane % half)
    q_sine = jnp.sin(q_angle)
    q_cos[...] = jnp.cos(q_angle)
    q_sin[...] = jnp.where(lane < half, -q_sine, q_sine)

    def wq_step(d):
        @pl.when(z >= d)
        def _():
            j = z - d
            wq_copy(wq_buf.at[j], j, True).wait_recv()

            @pl.when(z < nz - 1)
            def _():
                wq_copy(wq_buf.at[j], j, True).start()

                @pl.when(z == d)
                def _():
                    wo_own(True)

        @pl.when(z + d < nz)
        def _():
            j = z + d
            wq_copy(wq_buf.at[j], j, False).wait_recv()

            @pl.when(z > 0)
            def _():
                wq_copy(wq_buf.at[j], j, False).start()

                @pl.when(z + d == nz - 1)
                def _():
                    wo_own(False)

    def q_send(j):
        return remote(q_part.at[j], q_recv.at[f], s_q.at[j], r_q.at[f], (j, s))

    def q_project(j):
        q_part[j] = jnp.dot(h_buf[...], wq_buf[j], preferred_element_type=f32)

        @pl.when(j != f)
        def _():
            q_send(j).start()

    def q_step(d):
        @pl.when(z >= d)
        def _():
            q_project(z - d)

        @pl.when(z + d < nz)
        def _():
            q_project(z + d)

    wq_step(1)
    own_h.wait()
    own_wq.wait()
    own_wkv.wait()
    hid_wait()
    for c in range(WO_CHUNKS):
        wo_cross(z, c, own=True).start()
    for d in range(1, nz):
        wkv_wait(d)
    kv_part[...] = lax.dot_general(
        h_buf[...], wkv_buf[...], (((1,), (1,)), ((), ())), preferred_element_type=f32
    )

    def kvp_send(d):
        ff = lax.rem(f + d, nf)
        return remote(
            kv_part.at[tile(ff, sub)], kv_recv.at[f], s_kvp.at[d - 1], r_kvp.at[f], (ff, s)
        )

    def kvp_wait(d):
        ff = lax.rem(f + d, nf)
        remote(
            kv_part.at[tile(ff, sub)], kv_recv.at[ff], s_kvp.at[d - 1], r_kvp.at[ff], here
        ).wait_recv()

    for d in range(1, nf):
        kvp_send(d).start()
    if nz > 2:
        wq_step(2)
    q_project(z)
    q_step(1)
    total = kv_part[tile(f, sub), :]
    for d in range(1, nf):
        kvp_wait(d)
        total = total + kv_recv[lax.rem(f + d, nf)]
    partner = jnp.where(
        lane < quarter, pltpu.roll(total, HD - quarter, 1), pltpu.roll(total, quarter, 1)
    )
    kv_piece[...] = (total * kv_cos + partner * kv_sin).astype(bf16)
    piece_rows = tile(f, sub)
    own_piece = pltpu.make_async_copy(kv_piece, kv_all.at[1, x, piece_rows], s_loc.at[5])
    own_piece.start()

    def kv_send(plane, dx, d):
        ff, xx = lax.rem(f + d, nf), lax.rem(x + dx, nx)
        slot = kv_all.at[plane, x, piece_rows]
        return remote(
            kv_piece if plane else slot, slot,
            s_kv.at[plane, dx, d], r_kv.at[plane, x, f], dev(ff, z, xx),
        )

    def kv_next():
        return remote(
            kv_piece, kv_all.at[0, x, piece_rows],
            s_kv.at[0, 0, 0], r_kv.at[0, x, f], dev(f, z + 1, x),
        )

    def kv_wait(plane, dx, d):
        ff, xx = lax.rem(f + d, nf), lax.rem(x + dx, nx)
        remote(
            kv_piece, kv_all.at[plane, xx, tile(ff, sub)],
            s_kv.at[plane, dx, d], r_kv.at[plane, xx, ff], here,
        ).wait_recv()

    pairs = [(dx, d) for dx in range(nx) for d in range(nf)]
    for pair in pairs[1:]:
        kv_send(1, *pair).start()

    @pl.when(z < nz - 1)
    def _():
        kv_next().start()

    q_step(2)

    @pl.when(z > 0)
    def _():
        kv_wait(0, 0, 0)
        for pair in pairs[1:]:
            kv_send(0, *pair).start()

    for d in range(3, nz):
        wq_step(d)
        q_step(d)

    def wo_side(j, to_right):
        for c in range(WO_CHUNKS):
            wo_wait(j, x, c)
            wo_copy(j, c, to_right).start()
            wo_cross(j, c).start()

    def wo_mid(d):
        @pl.when((z >= d) & (z < nz - 1))
        def _():
            wo_side(z - d, True)

        @pl.when((z + d < nz) & (z > 0))
        def _():
            wo_side(z + d, False)

    def wo_end(d, c):
        for end, j in ((0, d), (nz - 1, nz - 1 - d)):
            @pl.when(z == end)
            def _():
                wo_wait(j, x, c)
                wo_cross(j, c).start()

    for d in range(1, nz - 1):
        wo_mid(d)

    q_total = q_part[f]
    for d in range(1, nf):
        ff = lax.rem(f + d, nf)
        remote(q_part.at[0], q_recv.at[ff], s_q.at[0], r_q.at[ff], here).wait_recv()
        q_total = q_total + q_recv[ff]
    q_turned = q_total * q_cos[...] + pltpu.roll(q_total, half, 1) * q_sin[...]
    q_head = q_turned.astype(bf16).astype(f32)
    quarters = []
    for xx in range(nx):
        low = q_head if xx == 0 else pltpu.roll(q_head, HD - xx * quarter, 1)
        high = pltpu.roll(q_head, (HD - half - xx * quarter + quarter) % HD, 1)
        picked = jnp.where(lane < quarter, low, jnp.where(lane < half, high, 0.0))
        quarters.append(picked.astype(bf16))

    own_seg.wait()
    seg_wait = lambda plane, xx: remote(
        seg, seg_buf.at[plane, xx], s_seg.at[0], r_seg.at[plane, xx], here
    ).wait_recv()
    seg_wait(1, other)
    own_piece.wait()
    for pair in pairs[1:]:
        kv_wait(1, *pair)

    @pl.when(z > 0)
    def _():
        for xx in range(nx):
            seg_wait(0, xx)
        for pair in pairs[1:]:
            kv_wait(0, *pair)

    key_seg = jnp.concatenate(
        [seg_buf[plane, xx] for plane in range(2) for xx in range(nx)], axis=1
    )
    own_seg_row = key_seg[:, rows:]
    seg_column = jnp.transpose(jnp.broadcast_to(own_seg_row, (HD, rows)))[:, :1]
    key_pos = lax.broadcasted_iota(jnp.int32, (1, 2 * rows), 1) - rows
    keys = [
        jnp.concatenate([kv_all[0, xx], kv_all[1, xx]], axis=0) for xx in range(nx)
    ]
    step_rows = rows // nf
    for b in range(nf):
        span = slice(b * step_rows, (b + 1) * step_rows)
        query_pos = b * step_rows + lax.broadcasted_iota(jnp.int32, (step_rows, 1), 0)
        score = None
        for xx in range(nx):
            term = lax.dot_general(
                quarters[xx][span], keys[xx], (((1,), (1,)), ((), ())),
                preferred_element_type=f32,
            )
            score = term if score is None else score + term
        allowed = (key_pos <= query_pos) & (key_seg == seg_column[span])
        masked = jnp.where(allowed, score * HD ** (-0.5), NEG_FILL)
        row_max = jnp.max(masked, axis=1, keepdims=True)
        weight = jnp.where(allowed, jnp.exp(masked - row_max), 0.0)
        row_total = jnp.sum(weight, axis=1, keepdims=True)
        rounded = weight.astype(bf16)
        product = [
            jnp.dot(rounded, keys[xx], preferred_element_type=f32) for xx in range(nx)
        ]
        mixed = None
        for xx in reversed(range(nx)):
            low = pltpu.roll(product[xx], (half + xx * quarter) % HD, 1)
            high = pltpu.roll(product[xx], (HD - (nx - 1 - xx) * quarter) % HD, 1)
            lane_block = lane // quarter
            value = jnp.where(lane_block < nx, low, high)
            mixed = value if mixed is None else jnp.where(lane_block % nx == xx, value, mixed)
        mix_own[span, :] = (mixed / row_total).astype(bf16)
        for c in range(b * WO_CHUNKS // nf, (b + 1) * WO_CHUNKS // nf):
            wo_end(1, c)

    head = f * nx + x

    def mix_send(dx, d):
        ff, xx = lax.rem(f + d, nf), lax.rem(x + dx, nx)
        return remote(
            mix_own.at[tile(xx, tok)], mix_buf.at[:, tile(head, HD)],
            s_mix.at[dx, d], r_mix.at[x, f], dev(ff, z, xx),
        )

    def mix_wait(dx, d):
        ff, xx = lax.rem(f + d, nf), lax.rem(x + dx, nx)
        remote(
            mix_own.at[tile(x, tok)], mix_buf.at[:, tile(ff * nx + xx, HD)],
            s_mix.at[dx, d], r_mix.at[xx, ff], here,
        ).wait_recv()

    for pair in pairs[1:]:
        mix_send(*pair).start()
    own_mix = pltpu.make_async_copy(
        mix_own.at[tile(x, tok)], mix_buf.at[:, tile(head, HD)], s_loc.at[6]
    )
    own_mix.start()
    for d in range(2, nz - 1):
        for c in range(WO_CHUNKS):
            wo_end(d, c)
    own_mix.wait()
    own_wo.wait()
    for pair in pairs[1:]:
        mix_wait(*pair)
    wo_end(nz - 1, 0)
    for c in range(WO_CHUNKS):
        if c + 1 < WO_CHUNKS:
            wo_end(nz - 1, c + 1)
        for j in range(nz):
            wo_wait(j, other, c)
        out[:, c * chunk : (c + 1) * chunk] = jnp.dot(
            mix_buf[...], wo_buf[:, c * chunk : (c + 1) * chunk], preferred_element_type=f32
        ).astype(bf16)

    hid_send.wait_send()
    seg_same.wait_send()
    for d in range(1, nz):
        wkv_send(d).wait_send()
    for d in range(1, nf):
        kvp_send(d).wait_send()
        q_send(lax.rem(f + d, nf)).wait_send()
    for pair in pairs[1:]:
        kv_send(1, *pair).wait_send()
        mix_send(*pair).wait_send()

    @pl.when(z < nz - 1)
    def _():
        for xx in range(nx):
            seg_next(xx).wait_send()
        kv_next().wait_send()

    @pl.when(z > 0)
    def _():
        for pair in pairs[1:]:
            kv_send(0, *pair).wait_send()

    for j in range(nz):
        for c in range(WO_CHUNKS):
            wo_cross(j, c).wait_send()

        @pl.when((z < nz - 1) & (z >= j))
        def _():
            wq_copy(wq, j, True).wait_send()
            for c in range(WO_CHUNKS):
                wo_copy(j, c, True).wait_send()

        @pl.when((z > 0) & (z <= j))
        def _():
            wq_copy(wq, j, False).wait_send()
            for c in range(WO_CHUNKS):
                wo_copy(j, c, False).wait_send()


def fused_on_device(nf, nz, nx, hidden, w_query, w_keyvalue, w_output, segment_ids):
    tok, kdim = hidden.shape
    cols = w_output.shape[1]
    rows = tok * nx
    sub = rows // nf
    kvw = w_keyvalue.shape[1]
    f32, bf16 = jnp.float32, jnp.bfloat16
    dma = pltpu.SemaphoreType.DMA
    vmem = pl.BlockSpec(memory_space=pltpu.VMEM)
    scratch = [
        pltpu.VMEM((rows, kdim), bf16),
        pltpu.VMEM((nz, kdim, HD), bf16),
        pltpu.VMEM((nz * kvw, kdim), bf16),
        pltpu.VMEM((nz * nx * HD, cols), bf16),
        pltpu.VMEM((2, nx, 1, tok), jnp.int32),
        pltpu.VMEM((nz, rows, HD), f32),
        pltpu.VMEM((nf, rows, HD), f32),
        pltpu.VMEM((rows, nz * kvw), f32),
        pltpu.VMEM((nf, sub, nz * kvw), f32),
        pltpu.VMEM((sub, HD), bf16),
        pltpu.VMEM((2, nx, rows, HD), bf16),
        pltpu.VMEM((rows, HD), bf16),
        pltpu.VMEM((tok, nz * nx * HD), bf16),
        pltpu.VMEM((rows, HD), f32),
        pltpu.VMEM((rows, HD), f32),
        dma((7,)), dma, dma, dma((1 + nx,)), dma((2, nx)),
        dma((nz,)), dma((nz,)), dma((nz,)), dma((nz,)), dma((nz,)),
        dma((nz,)), dma((nf,)), dma((nf,)), dma((nf,)),
        dma((2, nx, nf)), dma((2, nx, nf)),
        dma((nz, WO_CHUNKS)), dma((nz, WO_CHUNKS)), dma((nz, WO_CHUNKS)),
        dma((nz * nx, WO_CHUNKS)), dma((nx, nf)), dma((nx, nf)),
    ]
    return pl.pallas_call(
        functools.partial(fused_kernel, nf, nz, nx),
        out_shape=jax.ShapeDtypeStruct((tok, cols), bf16),
        in_specs=[vmem] * 5,
        out_specs=vmem,
        scratch_shapes=scratch,
        name="fused_sublayer",
        compiler_params=pltpu.CompilerParams(
            collective_id=0, has_side_effects=True, vmem_limit_bytes=60 * 1024 * 1024
        ),
    )(hidden, w_query, w_keyvalue.T, w_output, segment_ids.reshape(1, tok))


def solution(mesh):
    in_specs = (P("sp", "fsdp"), P("fsdp", "sp"), P("fsdp", "sp"), P("sp", "fsdp"), P("sp"))
    out_specs = P("sp", "fsdp")
    nf, sp = mesh.shape["fsdp"], mesh.shape["sp"]
    if sp == GROUP and sp == 2 * nf:
        body = functools.partial(fused_on_device, nf, nf, sp // nf)
    else:
        body = on_device
    return jax.shard_map(
        body, mesh=mesh, in_specs=in_specs, out_specs=out_specs, check_vma=False
    )
```

```python
import functools
import math

import jax
import jax.numpy as jnp
from jax import lax
from jax.experimental import pallas as pl
from jax.experimental.pallas import tpu as pltpu
from jax.sharding import PartitionSpec as P

HD = 128
GROUP = 8


ROPE_BASE = 500000.0
NEG_FILL = -1e30


def rotate(values, positions, head_count, width):
    row_count = values.shape[0]
    shaped = values.reshape(row_count, head_count, width)
    half_width = width // 2
    frequency = jnp.exp(
        jnp.arange(half_width, dtype=jnp.float32) * (-2.0 * math.log(ROPE_BASE) / width)
    )
    angles = positions.astype(jnp.float32)[:, None] * frequency[None, :]
    cosine = jnp.cos(angles)[:, None, :]
    sine_part = jnp.sin(angles)[:, None, :]
    lower_half = shaped[:, :, :half_width]
    upper_half = shaped[:, :, half_width:]
    turned = jnp.concatenate(
        [
            lower_half * cosine - upper_half * sine_part,
            upper_half * cosine + lower_half * sine_part,
        ],
        axis=2,
    )
    return turned.reshape(row_count, head_count * width)


def split_keys(kv_sum, positions, kv_count, width):
    row_count = kv_sum.shape[0]
    shaped = kv_sum.reshape(row_count, kv_count, 2, width)
    key_part = rotate(
        shaped[:, :, 0, :].reshape(row_count, kv_count * width), positions, kv_count, width
    )
    key_part = key_part.reshape(row_count, kv_count, 1, width)
    return jnp.concatenate([key_part, shaped[:, :, 1:2, :]], axis=2).astype(jnp.bfloat16)


def merge_keys(
    state_in, query_tile, query_pos_tile, query_seg_tile, key_tile, key_pos_tile, key_seg_tile
):
    running_max, running_sum, weighted = state_in
    allowed = (key_pos_tile[None, :] <= query_pos_tile[:, None]) & (
        key_seg_tile[None, :] == query_seg_tile[:, None]
    )
    key_part = key_tile[:, :HD]
    value_part = key_tile[:, HD:]
    scores = lax.dot_general(
        query_tile, key_part, (((1,), (1,)), ((), ())), preferred_element_type=jnp.float32
    ) * HD ** (-0.5)
    masked = jnp.where(allowed, scores, NEG_FILL)
    new_max = jnp.maximum(running_max, jnp.max(masked, axis=1))
    weights = jnp.where(allowed, jnp.exp(masked - new_max[:, None]), 0.0)
    new_sum = jnp.sum(weights, axis=1)
    new_weighted = jnp.dot(
        weights.astype(jnp.bfloat16), value_part, preferred_element_type=jnp.float32
    )
    return (new_max, new_sum, new_weighted)


def on_device(hidden, w_query, w_keyvalue, w_output, segment_ids):
    fsdp_count = lax.axis_size("fsdp")
    seq_count = lax.axis_size("sp")
    fsdp_index = lax.axis_index("fsdp")
    seq_index = lax.axis_index("sp")
    tok_rows = hidden.shape[0]
    sub_rows = tok_rows // fsdp_count
    kv_count = seq_count // GROUP
    query_rows = seq_count * sub_rows
    offsets = jnp.arange(query_rows, dtype=jnp.int32)
    query_pos = offsets // sub_rows * tok_rows + fsdp_index * sub_rows + offsets % sub_rows
    own_positions = (
        seq_index * tok_rows + fsdp_index * sub_rows + jnp.arange(sub_rows, dtype=jnp.int32)
    )

    def project(weight_block):
        return jnp.dot(hidden, weight_block, preferred_element_type=jnp.float32)

    query_part = project(lax.all_gather(w_query, "sp", axis=1, tiled=True))
    kv_part = project(lax.all_gather(w_keyvalue, "sp", axis=1, tiled=True))
    query_sum, kv_sum = (
        lax.psum_scatter(query_part, "fsdp", scatter_dimension=0, tiled=True),
        lax.psum_scatter(kv_part, "fsdp", scatter_dimension=0, tiled=True),
    )
    query_local = rotate(query_sum, own_positions, seq_count, HD).astype(jnp.bfloat16)
    pairs = split_keys(kv_sum, own_positions, kv_count, HD)
    expanded = jnp.repeat(pairs, GROUP, axis=1).reshape(sub_rows, seq_count * 2 * HD)
    query_head, kv_head = (
        lax.all_to_all(query_local, "sp", split_axis=1, concat_axis=0, tiled=True),
        lax.all_to_all(expanded, "sp", split_axis=1, concat_axis=0, tiled=True),
    )
    segment_all = lax.all_gather(segment_ids, "sp", axis=0, tiled=True)
    query_seg = segment_all[query_pos]
    initial = (
        jnp.full((query_rows,), NEG_FILL, jnp.float32),
        jnp.zeros((query_rows,), jnp.float32),
        jnp.zeros((query_rows, HD), jnp.float32),
    )
    block_keys = lax.all_gather(kv_head, "fsdp", axis=0, tiled=True)
    piece_rows = block_keys.shape[0]
    row_ids = jnp.arange(piece_rows, dtype=jnp.int32)
    source_id = row_ids // query_rows
    within = row_ids % query_rows
    key_pos = within // sub_rows * tok_rows + source_id * sub_rows + within % sub_rows
    key_seg = segment_all[key_pos]
    final_max, final_sum, final_weighted = merge_keys(
        initial, query_head, query_pos, query_seg, block_keys, key_pos, key_seg
    )
    attention = (final_weighted / final_sum[:, None]).astype(jnp.bfloat16)
    back_rows = lax.all_to_all(attention, "sp", split_axis=0, concat_axis=1, tiled=True)
    mixed_rows = lax.all_gather(back_rows, "fsdp", axis=0, tiled=True)
    result = jnp.dot(
        mixed_rows,
        lax.all_gather(w_output, "sp", axis=0, tiled=True),
        preferred_element_type=jnp.float32,
    )
    return result.astype(jnp.bfloat16)


NEG_POS = -1
WO_CHUNKS = 4


def fused_kernel(
    nf, nz, nx, hid, wq, wkv, wo, seg, out,
    h_buf, wq_buf, wkv_buf, wo_buf, seg_buf,
    q_part, q_recv, kv_part, kv_recv, kv_piece, kv_all, mix_own, mix_buf, q_cos, q_sin,
    s_loc, s_hid, r_hid, s_seg, r_seg, s_wkv, r_wkv, s_wqr, s_wql, r_wq,
    s_q, r_q, s_kvp, r_kvp, s_kv, r_kv, s_wor, s_wol, s_wox, r_wo, s_mix, r_mix,
):
    f = lax.axis_index("fsdp")
    s = lax.axis_index("sp")
    z, x = s // nx, s % nx
    tok, kdim = hid.shape
    rows = tok * nx
    sub = rows // nf
    kvw = wkv.shape[0]
    other = 1 - x
    chunk = wo.shape[1] // WO_CHUNKS
    f32, bf16 = jnp.float32, jnp.bfloat16

    def dev(ff, zz, xx):
        return (ff, zz * nx + xx)

    def remote(src, dst, ss, rs, target):
        return pltpu.make_async_remote_copy(
            src_ref=src, dst_ref=dst, send_sem=ss, recv_sem=rs,
            device_id=target, device_id_type=pl.DeviceIdType.MESH,
        )

    def tile(ref, count):
        return pl.ds(pl.multiple_of(ref * count, count), count)

    here = (f, s)
    own_h = pltpu.make_async_copy(hid, h_buf.at[tile(x, tok)], s_loc.at[0])
    own_wq = pltpu.make_async_copy(wq, wq_buf.at[z], s_loc.at[1])
    own_wkv = pltpu.make_async_copy(wkv, wkv_buf.at[tile(z, kvw)], s_loc.at[2])
    own_wo = pltpu.make_async_copy(wo, wo_buf.at[tile(s, HD)], s_loc.at[3])
    own_seg = pltpu.make_async_copy(seg, seg_buf.at[1, x], s_loc.at[4])
    hid_send = remote(hid, h_buf.at[tile(x, tok)], s_hid, r_hid, dev(f, z, other))

    def hid_wait():
        remote(hid, h_buf.at[tile(other, tok)], s_hid, r_hid, here).wait_recv()

    def wkv_send(d):
        zz = lax.rem(z + d, nz)
        return remote(
            wkv, wkv_buf.at[tile(z, kvw)], s_wkv.at[d - 1], r_wkv.at[z], dev(f, zz, x)
        )

    def wkv_wait(d):
        zz = lax.rem(z + d, nz)
        remote(
            wkv, wkv_buf.at[tile(zz, kvw)], s_wkv.at[d - 1], r_wkv.at[zz], here
        ).wait_recv()

    def wq_copy(src, j, to_right):
        sems = s_wqr if to_right else s_wql
        return remote(
            src, wq_buf.at[j], sems.at[j], r_wq.at[j],
            dev(f, z + 1 if to_right else z - 1, x),
        )

    def wo_slice(zz, xx, c):
        return wo_buf.at[tile(zz * nx + xx, HD), c * chunk : (c + 1) * chunk]

    def wo_src(j, c, own):
        return wo.at[:, c * chunk : (c + 1) * chunk] if own else wo_slice(j, x, c)

    def wo_copy(j, c, to_right, own=False):
        sems = s_wor if to_right else s_wol
        return remote(
            wo_src(j, c, own), wo_slice(j, x, c), sems.at[j, c], r_wo.at[j * nx + x, c],
            dev(f, z + 1 if to_right else z - 1, x),
        )

    def wo_cross(j, c, own=False):
        return remote(
            wo_src(j, c, own), wo_slice(j, x, c), s_wox.at[j, c], r_wo.at[j * nx + x, c],
            dev(f, z, other),
        )

    def wo_wait(j, xx, c):
        remote(
            wo_slice(j, xx, c), wo_slice(j, xx, c), s_wox.at[j, c], r_wo.at[j * nx + xx, c], here
        ).wait_recv()

    def wo_own(to_right):
        for c in range(WO_CHUNKS):
            wo_copy(z, c, to_right, own=True).start()

    seg_same = remote(seg, seg_buf.at[1, x], s_seg.at[0], r_seg.at[1, x], dev(f, z, other))

    def seg_next(xx):
        return remote(
            seg, seg_buf.at[0, x], s_seg.at[1 + xx], r_seg.at[0, x], dev(f, z + 1, xx)
        )

    barrier = pltpu.get_barrier_semaphore()

    def greet(ff, zz, xx):
        pl.semaphore_signal(
            barrier, inc=1, device_id=dev(ff, zz, xx), device_id_type=pl.DeviceIdType.MESH
        )

    plane = nf * nx
    for step in (1, -1):
        @pl.when((z + step >= 0) & (z + step < nz))
        def _():
            for xx in range(nx):
                for ff in range(nf):
                    greet(ff, z + step, xx)

        for far in range(2, nz):
            @pl.when((z + far * step >= 0) & (z + far * step < nz))
            def _():
                greet(f, z + far * step, x)

    for d in range(1, plane):
        greet(lax.rem(f + d, nf), z, lax.rem(x + d // nf, nx))
    ends = jnp.where(z == 0, 1, 0) + jnp.where(z == nz - 1, 1, 0)
    pl.semaphore_wait(barrier, (3 - ends) * plane - 1 + nz - 3 + ends)

    for d in range(1, nz):
        wkv_send(d).start()

    @pl.when(z < nz - 1)
    def _():
        wq_copy(wq, z, True).start()

    @pl.when(z > 0)
    def _():
        wq_copy(wq, z, False).start()

    @pl.when(z == nz - 2)
    def _():
        wo_own(True)

    @pl.when(z == 1)
    def _():
        wo_own(False)

    hid_send.start()
    seg_same.start()

    @pl.when(z < nz - 1)
    def _():
        for xx in range(nx):
            seg_next(xx).start()

    for copy in (own_h, own_wq, own_wkv, own_wo, own_seg):
        copy.start()

    @pl.when(z == 0)
    def _():
        wo_own(True)
        kv_all[0] = jnp.zeros(kv_all.shape[1:], bf16)
        seg_buf[0] = jnp.full(seg_buf.shape[1:], NEG_POS, jnp.int32)

    @pl.when(z == nz - 1)
    def _():
        wo_own(False)

    def table(row_count, first, lane_index):
        position = (first + lax.broadcasted_iota(jnp.int32, (row_count, HD), 0)).astype(f32)
        frequency = jnp.exp(lane_index.astype(f32) * (-2.0 * math.log(ROPE_BASE) / HD))
        return position * frequency

    lane = lax.broadcasted_iota(jnp.int32, (1, HD), 1)
    half = HD // 2
    quarter = half // nx
    kv_angle = table(sub, z * rows + f * sub, x * quarter + lane % quarter)
    is_key = lane < half
    kv_cos = jnp.where(is_key, jnp.cos(kv_angle), 1.0)
    kv_sin = jnp.where(is_key, jnp.sin(kv_angle), 0.0)
    kv_sin = jnp.where(lane < quarter, -kv_sin, kv_sin)
    q_angle = table(rows, z * rows, lane % half)
    q_sine = jnp.sin(q_angle)
    q_cos[...] = jnp.cos(q_angle)
    q_sin[...] = jnp.where(lane < half, -q_sine, q_sine)

    def wq_step(d):
        @pl.when(z >= d)
        def _():
            j = z - d
            wq_copy(wq_buf.at[j], j, True).wait_recv()

            @pl.when(z < nz - 1)
            def _():
                wq_copy(wq_buf.at[j], j, True).start()

                @pl.when((z == d) & (z != nz - 2))
                def _():
                    wo_own(True)

        @pl.when(z + d < nz)
        def _():
            j = z + d
            wq_copy(wq_buf.at[j], j, False).wait_recv()

            @pl.when(z > 0)
            def _():
                wq_copy(wq_buf.at[j], j, False).start()

                @pl.when((z + d == nz - 1) & (z != 1))
                def _():
                    wo_own(False)

    def q_send(j):
        return remote(q_part.at[j], q_recv.at[f], s_q.at[j], r_q.at[f], (j, s))

    def q_project(j):
        q_part[j] = jnp.dot(h_buf[...], wq_buf[j], preferred_element_type=f32)

        @pl.when(j != f)
        def _():
            q_send(j).start()

    def q_step(d):
        @pl.when(z >= d)
        def _():
            q_project(z - d)

        @pl.when(z + d < nz)
        def _():
            q_project(z + d)

    def wo_end(d, c):
        for end, j in ((0, d), (nz - 1, nz - 1 - d)):
            @pl.when(z == end)
            def _():
                wo_wait(j, x, c)
                wo_cross(j, c).start()

    wq_step(1)
    own_h.wait()
    own_wq.wait()
    own_wkv.wait()
    hid_wait()
    for c in range(WO_CHUNKS):
        wo_cross(z, c, own=True).start()
    for d in range(1, nz):
        wkv_wait(d)
    kv_part[...] = lax.dot_general(
        h_buf[...], wkv_buf[...], (((1,), (1,)), ((), ())), preferred_element_type=f32
    )

    def kvp_send(d):
        ff = lax.rem(f + d, nf)
        return remote(
            kv_part.at[tile(ff, sub)], kv_recv.at[f], s_kvp.at[d - 1], r_kvp.at[f], (ff, s)
        )

    def kvp_wait(d):
        ff = lax.rem(f + d, nf)
        remote(
            kv_part.at[tile(ff, sub)], kv_recv.at[ff], s_kvp.at[d - 1], r_kvp.at[ff], here
        ).wait_recv()

    for d in range(1, nf):
        kvp_send(d).start()
    inner = (z > 0) & (z < nz - 1)

    @pl.when(inner)
    def _():
        wq_step(2)

    q_project(z)
    q_step(1)
    total = kv_part[tile(f, sub), :]
    for d in range(1, nf):
        kvp_wait(d)
        total = total + kv_recv[lax.rem(f + d, nf)]
    partner = jnp.where(
        lane < quarter, pltpu.roll(total, HD - quarter, 1), pltpu.roll(total, quarter, 1)
    )
    kv_piece[...] = (total * kv_cos + partner * kv_sin).astype(bf16)
    piece_rows = tile(f, sub)
    own_piece = pltpu.make_async_copy(kv_piece, kv_all.at[1, x, piece_rows], s_loc.at[5])
    own_piece.start()

    def kv_send(plane, dx, d):
        ff, xx = lax.rem(f + d, nf), lax.rem(x + dx, nx)
        slot = kv_all.at[plane, x, piece_rows]
        return remote(
            kv_piece if plane else slot, slot,
            s_kv.at[plane, dx, d], r_kv.at[plane, x, f], dev(ff, z, xx),
        )

    def kv_next():
        return remote(
            kv_piece, kv_all.at[0, x, piece_rows],
            s_kv.at[0, 0, 0], r_kv.at[0, x, f], dev(f, z + 1, x),
        )

    def kv_wait(plane, dx, d):
        ff, xx = lax.rem(f + d, nf), lax.rem(x + dx, nx)
        remote(
            kv_piece, kv_all.at[plane, xx, tile(ff, sub)],
            s_kv.at[plane, dx, d], r_kv.at[plane, xx, ff], here,
        ).wait_recv()

    pairs = [(dx, d) for dx in range(nx) for d in range(nf)]
    for pair in pairs[1:]:
        kv_send(1, *pair).start()

    @pl.when(z < nz - 1)
    def _():
        kv_next().start()

    for c in range(WO_CHUNKS):
        wo_end(1, c)

    @pl.when(jnp.logical_not(inner))
    def _():
        wq_step(2)

    q_step(2)

    @pl.when(z > 0)
    def _():
        kv_wait(0, 0, 0)
        for pair in pairs[1:]:
            kv_send(0, *pair).start()

    for d in range(3, nz):
        wq_step(d)
        q_step(d)

    def wo_side(j, to_right):
        for c in range(WO_CHUNKS):
            wo_wait(j, x, c)
            wo_copy(j, c, to_right).start()
            wo_cross(j, c).start()

    def wo_mid(d):
        @pl.when((z >= d) & (z < nz - 1))
        def _():
            wo_side(z - d, True)

        @pl.when((z + d < nz) & (z > 0))
        def _():
            wo_side(z + d, False)

    for d in range(1, nz - 1):
        wo_mid(d)

    q_total = q_part[f]
    for d in range(1, nf):
        ff = lax.rem(f + d, nf)
        remote(q_part.at[0], q_recv.at[ff], s_q.at[0], r_q.at[ff], here).wait_recv()
        q_total = q_total + q_recv[ff]
    q_turned = q_total * q_cos[...] + pltpu.roll(q_total, half, 1) * q_sin[...]
    q_head = q_turned.astype(bf16).astype(f32)
    quarters = []
    for xx in range(nx):
        low = q_head if xx == 0 else pltpu.roll(q_head, HD - xx * quarter, 1)
        high = pltpu.roll(q_head, (HD - half - xx * quarter + quarter) % HD, 1)
        picked = jnp.where(lane < quarter, low, jnp.where(lane < half, high, 0.0))
        quarters.append(picked.astype(bf16))

    own_seg.wait()
    seg_wait = lambda plane, xx: remote(
        seg, seg_buf.at[plane, xx], s_seg.at[0], r_seg.at[plane, xx], here
    ).wait_recv()
    seg_wait(1, other)
    own_piece.wait()
    for pair in pairs[1:]:
        kv_wait(1, *pair)

    @pl.when(z > 0)
    def _():
        for xx in range(nx):
            seg_wait(0, xx)
        for pair in pairs[1:]:
            kv_wait(0, *pair)

    key_seg = jnp.concatenate(
        [seg_buf[plane, xx] for plane in range(2) for xx in range(nx)], axis=1
    )
    own_seg_row = key_seg[:, rows:]
    seg_column = jnp.transpose(jnp.broadcast_to(own_seg_row, (HD, rows)))[:, :1]
    key_pos = lax.broadcasted_iota(jnp.int32, (1, 2 * rows), 1) - rows
    keys = [
        jnp.concatenate([kv_all[0, xx], kv_all[1, xx]], axis=0) for xx in range(nx)
    ]
    step_rows = rows // nf
    for b in range(nf):
        span = slice(b * step_rows, (b + 1) * step_rows)
        query_pos = b * step_rows + lax.broadcasted_iota(jnp.int32, (step_rows, 1), 0)
        score = None
        for xx in range(nx):
            term = lax.dot_general(
                quarters[xx][span], keys[xx], (((1,), (1,)), ((), ())),
                preferred_element_type=f32,
            )
            score = term if score is None else score + term
        allowed = (key_pos <= query_pos) & (key_seg == seg_column[span])
        masked = jnp.where(allowed, score * HD ** (-0.5), NEG_FILL)
        row_max = jnp.max(masked, axis=1, keepdims=True)
        weight = jnp.where(allowed, jnp.exp(masked - row_max), 0.0)
        row_total = jnp.sum(weight, axis=1, keepdims=True)
        rounded = weight.astype(bf16)
        product = [
            jnp.dot(rounded, keys[xx], preferred_element_type=f32) for xx in range(nx)
        ]
        mixed = None
        for xx in reversed(range(nx)):
            low = pltpu.roll(product[xx], (half + xx * quarter) % HD, 1)
            high = pltpu.roll(product[xx], (HD - (nx - 1 - xx) * quarter) % HD, 1)
            lane_block = lane // quarter
            value = jnp.where(lane_block < nx, low, high)
            mixed = value if mixed is None else jnp.where(lane_block % nx == xx, value, mixed)
        mix_own[span, :] = (mixed / row_total).astype(bf16)

    head = f * nx + x

    def mix_send(dx, d):
        ff, xx = lax.rem(f + d, nf), lax.rem(x + dx, nx)
        return remote(
            mix_own.at[tile(xx, tok)], mix_buf.at[:, tile(head, HD)],
            s_mix.at[dx, d], r_mix.at[x, f], dev(ff, z, xx),
        )

    def mix_wait(dx, d):
        ff, xx = lax.rem(f + d, nf), lax.rem(x + dx, nx)
        remote(
            mix_own.at[tile(x, tok)], mix_buf.at[:, tile(ff * nx + xx, HD)],
            s_mix.at[dx, d], r_mix.at[xx, ff], here,
        ).wait_recv()

    for pair in pairs[1:]:
        mix_send(*pair).start()
    own_mix = pltpu.make_async_copy(
        mix_own.at[tile(x, tok)], mix_buf.at[:, tile(head, HD)], s_loc.at[6]
    )
    own_mix.start()
    for d in range(2, nz - 1):
        for c in range(WO_CHUNKS):
            wo_end(d, c)
    own_mix.wait()
    own_wo.wait()
    for pair in pairs[1:]:
        mix_wait(*pair)
    wo_end(nz - 1, 0)
    for c in range(WO_CHUNKS):
        if c + 1 < WO_CHUNKS:
            wo_end(nz - 1, c + 1)
        for j in range(nz):
            wo_wait(j, other, c)
        out[:, c * chunk : (c + 1) * chunk] = jnp.dot(
            mix_buf[...], wo_buf[:, c * chunk : (c + 1) * chunk], preferred_element_type=f32
        ).astype(bf16)

    hid_send.wait_send()
    seg_same.wait_send()
    for d in range(1, nz):
        wkv_send(d).wait_send()
    for d in range(1, nf):
        kvp_send(d).wait_send()
        q_send(lax.rem(f + d, nf)).wait_send()
    for pair in pairs[1:]:
        kv_send(1, *pair).wait_send()
        mix_send(*pair).wait_send()

    @pl.when(z < nz - 1)
    def _():
        for xx in range(nx):
            seg_next(xx).wait_send()
        kv_next().wait_send()

    @pl.when(z > 0)
    def _():
        for pair in pairs[1:]:
            kv_send(0, *pair).wait_send()

    for j in range(nz):
        for c in range(WO_CHUNKS):
            wo_cross(j, c).wait_send()

        @pl.when((z < nz - 1) & (z >= j))
        def _():
            wq_copy(wq, j, True).wait_send()
            for c in range(WO_CHUNKS):
                wo_copy(j, c, True).wait_send()

        @pl.when((z > 0) & (z <= j))
        def _():
            wq_copy(wq, j, False).wait_send()
            for c in range(WO_CHUNKS):
                wo_copy(j, c, False).wait_send()


def fused_on_device(nf, nz, nx, hidden, w_query, w_keyvalue, w_output, segment_ids):
    tok, kdim = hidden.shape
    cols = w_output.shape[1]
    rows = tok * nx
    sub = rows // nf
    kvw = w_keyvalue.shape[1]
    f32, bf16 = jnp.float32, jnp.bfloat16
    dma = pltpu.SemaphoreType.DMA
    vmem = pl.BlockSpec(memory_space=pltpu.VMEM)
    scratch = [
        pltpu.VMEM((rows, kdim), bf16),
        pltpu.VMEM((nz, kdim, HD), bf16),
        pltpu.VMEM((nz * kvw, kdim), bf16),
        pltpu.VMEM((nz * nx * HD, cols), bf16),
        pltpu.VMEM((2, nx, 1, tok), jnp.int32),
        pltpu.VMEM((nz, rows, HD), f32),
        pltpu.VMEM((nf, rows, HD), f32),
        pltpu.VMEM((rows, nz * kvw), f32),
        pltpu.VMEM((nf, sub, nz * kvw), f32),
        pltpu.VMEM((sub, HD), bf16),
        pltpu.VMEM((2, nx, rows, HD), bf16),
        pltpu.VMEM((rows, HD), bf16),
        pltpu.VMEM((tok, nz * nx * HD), bf16),
        pltpu.VMEM((rows, HD), f32),
        pltpu.VMEM((rows, HD), f32),
        dma((7,)), dma, dma, dma((1 + nx,)), dma((2, nx)),
        dma((nz,)), dma((nz,)), dma((nz,)), dma((nz,)), dma((nz,)),
        dma((nz,)), dma((nf,)), dma((nf,)), dma((nf,)),
        dma((2, nx, nf)), dma((2, nx, nf)),
        dma((nz, WO_CHUNKS)), dma((nz, WO_CHUNKS)), dma((nz, WO_CHUNKS)),
        dma((nz * nx, WO_CHUNKS)), dma((nx, nf)), dma((nx, nf)),
    ]
    return pl.pallas_call(
        functools.partial(fused_kernel, nf, nz, nx),
        out_shape=jax.ShapeDtypeStruct((tok, cols), bf16),
        in_specs=[vmem] * 5,
        out_specs=vmem,
        scratch_shapes=scratch,
        name="fused_sublayer",
        compiler_params=pltpu.CompilerParams(
            collective_id=0, has_side_effects=True, vmem_limit_bytes=60 * 1024 * 1024
        ),
    )(hidden, w_query, w_keyvalue.T, w_output, segment_ids.reshape(1, tok))


def solution(mesh):
    in_specs = (P("sp", "fsdp"), P("fsdp", "sp"), P("fsdp", "sp"), P("sp", "fsdp"), P("sp"))
    out_specs = P("sp", "fsdp")
    nf, sp = mesh.shape["fsdp"], mesh.shape["sp"]
    if sp == GROUP and sp == 2 * nf:
        body = functools.partial(fused_on_device, nf, nf, sp // nf)
    else:
        body = on_device
    return jax.shard_map(
        body, mesh=mesh, in_specs=in_specs, out_specs=out_specs, check_vma=False
    )
```

```python
import functools
import math

import jax
import jax.numpy as jnp
from jax import lax
from jax.experimental import pallas as pl
from jax.experimental.pallas import tpu as pltpu
from jax.sharding import PartitionSpec as P

HD = 128
GROUP = 8


ROPE_BASE = 500000.0
NEG_FILL = -1e30


def rotate(values, positions, head_count, width):
    row_count = values.shape[0]
    shaped = values.reshape(row_count, head_count, width)
    half_width = width // 2
    frequency = jnp.exp(
        jnp.arange(half_width, dtype=jnp.float32) * (-2.0 * math.log(ROPE_BASE) / width)
    )
    angles = positions.astype(jnp.float32)[:, None] * frequency[None, :]
    cosine = jnp.cos(angles)[:, None, :]
    sine_part = jnp.sin(angles)[:, None, :]
    lower_half = shaped[:, :, :half_width]
    upper_half = shaped[:, :, half_width:]
    turned = jnp.concatenate(
        [
            lower_half * cosine - upper_half * sine_part,
            upper_half * cosine + lower_half * sine_part,
        ],
        axis=2,
    )
    return turned.reshape(row_count, head_count * width)


def split_keys(kv_sum, positions, kv_count, width):
    row_count = kv_sum.shape[0]
    shaped = kv_sum.reshape(row_count, kv_count, 2, width)
    key_part = rotate(
        shaped[:, :, 0, :].reshape(row_count, kv_count * width), positions, kv_count, width
    )
    key_part = key_part.reshape(row_count, kv_count, 1, width)
    return jnp.concatenate([key_part, shaped[:, :, 1:2, :]], axis=2).astype(jnp.bfloat16)


def merge_keys(
    state_in, query_tile, query_pos_tile, query_seg_tile, key_tile, key_pos_tile, key_seg_tile
):
    running_max, running_sum, weighted = state_in
    allowed = (key_pos_tile[None, :] <= query_pos_tile[:, None]) & (
        key_seg_tile[None, :] == query_seg_tile[:, None]
    )
    key_part = key_tile[:, :HD]
    value_part = key_tile[:, HD:]
    scores = lax.dot_general(
        query_tile, key_part, (((1,), (1,)), ((), ())), preferred_element_type=jnp.float32
    ) * HD ** (-0.5)
    masked = jnp.where(allowed, scores, NEG_FILL)
    new_max = jnp.maximum(running_max, jnp.max(masked, axis=1))
    weights = jnp.where(allowed, jnp.exp(masked - new_max[:, None]), 0.0)
    new_sum = jnp.sum(weights, axis=1)
    new_weighted = jnp.dot(
        weights.astype(jnp.bfloat16), value_part, preferred_element_type=jnp.float32
    )
    return (new_max, new_sum, new_weighted)


def on_device(hidden, w_query, w_keyvalue, w_output, segment_ids):
    fsdp_count = lax.axis_size("fsdp")
    seq_count = lax.axis_size("sp")
    fsdp_index = lax.axis_index("fsdp")
    seq_index = lax.axis_index("sp")
    tok_rows = hidden.shape[0]
    sub_rows = tok_rows // fsdp_count
    kv_count = seq_count // GROUP
    query_rows = seq_count * sub_rows
    offsets = jnp.arange(query_rows, dtype=jnp.int32)
    query_pos = offsets // sub_rows * tok_rows + fsdp_index * sub_rows + offsets % sub_rows
    own_positions = (
        seq_index * tok_rows + fsdp_index * sub_rows + jnp.arange(sub_rows, dtype=jnp.int32)
    )

    def project(weight_block):
        return jnp.dot(hidden, weight_block, preferred_element_type=jnp.float32)

    query_part = project(lax.all_gather(w_query, "sp", axis=1, tiled=True))
    kv_part = project(lax.all_gather(w_keyvalue, "sp", axis=1, tiled=True))
    query_sum, kv_sum = (
        lax.psum_scatter(query_part, "fsdp", scatter_dimension=0, tiled=True),
        lax.psum_scatter(kv_part, "fsdp", scatter_dimension=0, tiled=True),
    )
    query_local = rotate(query_sum, own_positions, seq_count, HD).astype(jnp.bfloat16)
    pairs = split_keys(kv_sum, own_positions, kv_count, HD)
    expanded = jnp.repeat(pairs, GROUP, axis=1).reshape(sub_rows, seq_count * 2 * HD)
    query_head, kv_head = (
        lax.all_to_all(query_local, "sp", split_axis=1, concat_axis=0, tiled=True),
        lax.all_to_all(expanded, "sp", split_axis=1, concat_axis=0, tiled=True),
    )
    segment_all = lax.all_gather(segment_ids, "sp", axis=0, tiled=True)
    query_seg = segment_all[query_pos]
    initial = (
        jnp.full((query_rows,), NEG_FILL, jnp.float32),
        jnp.zeros((query_rows,), jnp.float32),
        jnp.zeros((query_rows, HD), jnp.float32),
    )
    block_keys = lax.all_gather(kv_head, "fsdp", axis=0, tiled=True)
    piece_rows = block_keys.shape[0]
    row_ids = jnp.arange(piece_rows, dtype=jnp.int32)
    source_id = row_ids // query_rows
    within = row_ids % query_rows
    key_pos = within // sub_rows * tok_rows + source_id * sub_rows + within % sub_rows
    key_seg = segment_all[key_pos]
    final_max, final_sum, final_weighted = merge_keys(
        initial, query_head, query_pos, query_seg, block_keys, key_pos, key_seg
    )
    attention = (final_weighted / final_sum[:, None]).astype(jnp.bfloat16)
    back_rows = lax.all_to_all(attention, "sp", split_axis=0, concat_axis=1, tiled=True)
    mixed_rows = lax.all_gather(back_rows, "fsdp", axis=0, tiled=True)
    result = jnp.dot(
        mixed_rows,
        lax.all_gather(w_output, "sp", axis=0, tiled=True),
        preferred_element_type=jnp.float32,
    )
    return result.astype(jnp.bfloat16)


NEG_POS = -1
WO_CHUNKS = 4


def fused_kernel(
    nf, nz, nx, hid, wq, wkv, wo, seg, out,
    h_buf, wq_buf, wkv_buf, wo_buf, seg_buf,
    q_part, q_recv, kv_part, kv_recv, kv_piece, kv_all, mix_own, mix_buf, q_cos, q_sin,
    s_loc, s_hid, r_hid, s_seg, r_seg, s_wkv, r_wkv, s_wqr, s_wql, r_wq,
    s_q, r_q, s_kvp, r_kvp, s_kv, r_kv, s_wor, s_wol, s_wox, r_wo, s_mix, r_mix,
):
    f = lax.axis_index("fsdp")
    s = lax.axis_index("sp")
    z, x = s // nx, s % nx
    tok, kdim = hid.shape
    rows = tok * nx
    sub = rows // nf
    kvw = wkv.shape[0]
    other = 1 - x
    chunk = wo.shape[1] // WO_CHUNKS
    f32, bf16 = jnp.float32, jnp.bfloat16

    def dev(ff, zz, xx):
        return (ff, zz * nx + xx)

    def remote(src, dst, ss, rs, target):
        return pltpu.make_async_remote_copy(
            src_ref=src, dst_ref=dst, send_sem=ss, recv_sem=rs,
            device_id=target, device_id_type=pl.DeviceIdType.MESH,
        )

    def tile(ref, count):
        return pl.ds(pl.multiple_of(ref * count, count), count)

    here = (f, s)
    own_h = pltpu.make_async_copy(hid, h_buf.at[tile(x, tok)], s_loc.at[0])
    own_wq = pltpu.make_async_copy(wq, wq_buf.at[z], s_loc.at[1])
    own_wkv = pltpu.make_async_copy(wkv, wkv_buf.at[tile(z, kvw)], s_loc.at[2])
    own_wo = pltpu.make_async_copy(wo, wo_buf.at[tile(s, HD)], s_loc.at[3])
    own_seg = pltpu.make_async_copy(seg, seg_buf.at[1, x], s_loc.at[4])
    hid_send = remote(hid, h_buf.at[tile(x, tok)], s_hid, r_hid, dev(f, z, other))

    def hid_wait():
        remote(hid, h_buf.at[tile(other, tok)], s_hid, r_hid, here).wait_recv()

    def wkv_send(d):
        zz = lax.rem(z + d, nz)
        return remote(
            wkv, wkv_buf.at[tile(z, kvw)], s_wkv.at[d - 1], r_wkv.at[z], dev(f, zz, x)
        )

    def wkv_wait(d):
        zz = lax.rem(z + d, nz)
        remote(
            wkv, wkv_buf.at[tile(zz, kvw)], s_wkv.at[d - 1], r_wkv.at[zz], here
        ).wait_recv()

    def wq_copy(src, j, to_right):
        sems = s_wqr if to_right else s_wql
        return remote(
            src, wq_buf.at[j], sems.at[j], r_wq.at[j],
            dev(f, z + 1 if to_right else z - 1, x),
        )

    def wo_slice(zz, xx, c):
        return wo_buf.at[tile(zz * nx + xx, HD), c * chunk : (c + 1) * chunk]

    def wo_src(j, c, own):
        return wo.at[:, c * chunk : (c + 1) * chunk] if own else wo_slice(j, x, c)

    def wo_copy(j, c, to_right, own=False):
        sems = s_wor if to_right else s_wol
        return remote(
            wo_src(j, c, own), wo_slice(j, x, c), sems.at[j, c], r_wo.at[j * nx + x, c],
            dev(f, z + 1 if to_right else z - 1, x),
        )

    def wo_cross(j, c, own=False):
        return remote(
            wo_src(j, c, own), wo_slice(j, x, c), s_wox.at[j, c], r_wo.at[j * nx + x, c],
            dev(f, z, other),
        )

    def wo_wait(j, xx, c):
        remote(
            wo_slice(j, xx, c), wo_slice(j, xx, c), s_wox.at[j, c], r_wo.at[j * nx + xx, c], here
        ).wait_recv()

    def wo_own(to_right):
        for c in range(WO_CHUNKS):
            wo_copy(z, c, to_right, own=True).start()

    seg_same = remote(seg, seg_buf.at[1, x], s_seg.at[0], r_seg.at[1, x], dev(f, z, other))

    def seg_next(xx):
        return remote(
            seg, seg_buf.at[0, x], s_seg.at[1 + xx], r_seg.at[0, x], dev(f, z + 1, xx)
        )

    barrier = pltpu.get_barrier_semaphore()

    def greet(ff, zz, xx):
        pl.semaphore_signal(
            barrier, inc=1, device_id=dev(ff, zz, xx), device_id_type=pl.DeviceIdType.MESH
        )

    plane = nf * nx
    for step in (1, -1):
        @pl.when((z + step >= 0) & (z + step < nz))
        def _():
            for xx in range(nx):
                for ff in range(nf):
                    greet(ff, z + step, xx)

        for far in range(2, nz):
            @pl.when((z + far * step >= 0) & (z + far * step < nz))
            def _():
                greet(f, z + far * step, x)

    for d in range(1, plane):
        greet(lax.rem(f + d, nf), z, lax.rem(x + d // nf, nx))
    ends = jnp.where(z == 0, 1, 0) + jnp.where(z == nz - 1, 1, 0)
    pl.semaphore_wait(barrier, (3 - ends) * plane - 1 + nz - 3 + ends)

    for d in range(1, nz):
        wkv_send(d).start()

    @pl.when(z < nz - 1)
    def _():
        wq_copy(wq, z, True).start()

    @pl.when(z > 0)
    def _():
        wq_copy(wq, z, False).start()

    @pl.when(z == nz - 2)
    def _():
        wo_own(True)

    @pl.when(z == 1)
    def _():
        wo_own(False)

    hid_send.start()
    seg_same.start()

    @pl.when(z < nz - 1)
    def _():
        for xx in range(nx):
            seg_next(xx).start()

    for copy in (own_h, own_wq, own_wkv, own_wo, own_seg):
        copy.start()

    @pl.when(z == 0)
    def _():
        wo_own(True)
        kv_all[0] = jnp.zeros(kv_all.shape[1:], bf16)
        seg_buf[0] = jnp.full(seg_buf.shape[1:], NEG_POS, jnp.int32)

    @pl.when(z == nz - 1)
    def _():
        wo_own(False)

    def table(row_count, first, lane_index):
        position = (first + lax.broadcasted_iota(jnp.int32, (row_count, HD), 0)).astype(f32)
        frequency = jnp.exp(lane_index.astype(f32) * (-2.0 * math.log(ROPE_BASE) / HD))
        return position * frequency

    lane = lax.broadcasted_iota(jnp.int32, (1, HD), 1)
    half = HD // 2
    quarter = half // nx
    kv_angle = table(sub, z * rows + f * sub, x * quarter + lane % quarter)
    is_key = lane < half
    kv_cos = jnp.where(is_key, jnp.cos(kv_angle), 1.0)
    kv_sin = jnp.where(is_key, jnp.sin(kv_angle), 0.0)
    kv_sin = jnp.where(lane < quarter, -kv_sin, kv_sin)
    q_angle = table(rows, z * rows, lane % half)
    q_sine = jnp.sin(q_angle)
    q_cos[...] = jnp.cos(q_angle)
    q_sin[...] = jnp.where(lane < half, -q_sine, q_sine)

    def wq_step(d):
        @pl.when(z >= d)
        def _():
            j = z - d
            wq_copy(wq_buf.at[j], j, True).wait_recv()

            @pl.when(z < nz - 1)
            def _():
                wq_copy(wq_buf.at[j], j, True).start()

                @pl.when((z == d) & (z != nz - 2))
                def _():
                    wo_own(True)

        @pl.when(z + d < nz)
        def _():
            j = z + d
            wq_copy(wq_buf.at[j], j, False).wait_recv()

            @pl.when(z > 0)
            def _():
                wq_copy(wq_buf.at[j], j, False).start()

                @pl.when((z + d == nz - 1) & (z != 1))
                def _():
                    wo_own(False)

    def q_send(j):
        return remote(q_part.at[j], q_recv.at[f], s_q.at[j], r_q.at[f], (j, s))

    def q_project(j):
        q_part[j] = jnp.dot(h_buf[...], wq_buf[j], preferred_element_type=f32)

        @pl.when(j != f)
        def _():
            q_send(j).start()

    def q_step(d):
        @pl.when(z >= d)
        def _():
            q_project(z - d)

        @pl.when(z + d < nz)
        def _():
            q_project(z + d)

    def wo_end(d, c):
        for end, j in ((0, d), (nz - 1, nz - 1 - d)):
            @pl.when(z == end)
            def _():
                wo_wait(j, x, c)
                wo_cross(j, c).start()

    wq_step(1)
    own_h.wait()
    own_wq.wait()
    own_wkv.wait()
    hid_wait()
    for c in range(WO_CHUNKS):
        wo_cross(z, c, own=True).start()
    for d in range(1, nz):
        wkv_wait(d)
    kv_part[...] = lax.dot_general(
        h_buf[...], wkv_buf[...], (((1,), (1,)), ((), ())), preferred_element_type=f32
    )

    def kvp_send(d):
        ff = lax.rem(f + d, nf)
        return remote(
            kv_part.at[tile(ff, sub)], kv_recv.at[f], s_kvp.at[d - 1], r_kvp.at[f], (ff, s)
        )

    def kvp_wait(d):
        ff = lax.rem(f + d, nf)
        remote(
            kv_part.at[tile(ff, sub)], kv_recv.at[ff], s_kvp.at[d - 1], r_kvp.at[ff], here
        ).wait_recv()

    for d in range(1, nf):
        kvp_send(d).start()
    inner = (z > 0) & (z < nz - 1)

    @pl.when(inner)
    def _():
        wq_step(2)

    q_project(z)
    q_step(1)
    total = kv_part[tile(f, sub), :]
    for d in range(1, nf):
        kvp_wait(d)
        total = total + kv_recv[lax.rem(f + d, nf)]
    partner = jnp.where(
        lane < quarter, pltpu.roll(total, HD - quarter, 1), pltpu.roll(total, quarter, 1)
    )
    kv_piece[...] = (total * kv_cos + partner * kv_sin).astype(bf16)
    piece_rows = tile(f, sub)
    own_piece = pltpu.make_async_copy(kv_piece, kv_all.at[1, x, piece_rows], s_loc.at[5])
    own_piece.start()

    def kv_send(plane, dx, d):
        ff, xx = lax.rem(f + d, nf), lax.rem(x + dx, nx)
        slot = kv_all.at[plane, x, piece_rows]
        return remote(
            kv_piece if plane else slot, slot,
            s_kv.at[plane, dx, d], r_kv.at[plane, x, f], dev(ff, z, xx),
        )

    def kv_next():
        return remote(
            kv_piece, kv_all.at[0, x, piece_rows],
            s_kv.at[0, 0, 0], r_kv.at[0, x, f], dev(f, z + 1, x),
        )

    def kv_wait(plane, dx, d):
        ff, xx = lax.rem(f + d, nf), lax.rem(x + dx, nx)
        remote(
            kv_piece, kv_all.at[plane, xx, tile(ff, sub)],
            s_kv.at[plane, dx, d], r_kv.at[plane, xx, ff], here,
        ).wait_recv()

    pairs = [(dx, d) for dx in range(nx) for d in range(nf)]
    for pair in pairs[1:]:
        kv_send(1, *pair).start()

    @pl.when(z < nz - 1)
    def _():
        kv_next().start()

    for c in range(WO_CHUNKS):
        wo_end(1, c)

    @pl.when(jnp.logical_not(inner))
    def _():
        wq_step(2)

    q_step(2)

    @pl.when(z > 0)
    def _():
        kv_wait(0, 0, 0)
        for pair in pairs[1:]:
            kv_send(0, *pair).start()

    for d in range(3, nz):
        wq_step(d)
        q_step(d)

    def wo_side(j, to_right):
        for c in range(WO_CHUNKS):
            wo_wait(j, x, c)
            wo_copy(j, c, to_right).start()
            wo_cross(j, c).start()

    def wo_mid(d):
        @pl.when((z >= d) & (z < nz - 1))
        def _():
            wo_side(z - d, True)

        @pl.when((z + d < nz) & (z > 0))
        def _():
            wo_side(z + d, False)

    for d in range(1, nz - 1):
        wo_mid(d)

    q_total = q_part[f]
    for d in range(1, nf):
        ff = lax.rem(f + d, nf)
        remote(q_part.at[0], q_recv.at[ff], s_q.at[0], r_q.at[ff], here).wait_recv()
        q_total = q_total + q_recv[ff]
    q_turned = q_total * q_cos[...] + pltpu.roll(q_total, half, 1) * q_sin[...]
    q_head = q_turned.astype(bf16).astype(f32)
    quarters = []
    for xx in range(nx):
        low = q_head if xx == 0 else pltpu.roll(q_head, HD - xx * quarter, 1)
        high = pltpu.roll(q_head, (HD - half - xx * quarter + quarter) % HD, 1)
        picked = jnp.where(lane < quarter, low, jnp.where(lane < half, high, 0.0))
        quarters.append(picked.astype(bf16))

    own_seg.wait()
    seg_wait = lambda plane, xx: remote(
        seg, seg_buf.at[plane, xx], s_seg.at[0], r_seg.at[plane, xx], here
    ).wait_recv()
    seg_wait(1, other)
    own_piece.wait()
    for pair in pairs[1:]:
        kv_wait(1, *pair)

    @pl.when(z > 0)
    def _():
        for xx in range(nx):
            seg_wait(0, xx)
        for pair in pairs[1:]:
            kv_wait(0, *pair)

    key_seg = jnp.concatenate(
        [seg_buf[plane, xx] for plane in range(2) for xx in range(nx)], axis=1
    )
    own_seg_row = key_seg[:, rows:]
    seg_column = jnp.transpose(jnp.broadcast_to(own_seg_row, (HD, rows)))[:, :1]
    key_pos = lax.broadcasted_iota(jnp.int32, (1, 2 * rows), 1) - rows
    keys = [
        jnp.concatenate([kv_all[0, xx], kv_all[1, xx]], axis=0) for xx in range(nx)
    ]
    step_rows = rows // nf
    for b in range(nf):
        span = slice(b * step_rows, (b + 1) * step_rows)
        query_pos = b * step_rows + lax.broadcasted_iota(jnp.int32, (step_rows, 1), 0)
        score = None
        for xx in range(nx):
            term = lax.dot_general(
                quarters[xx][span], keys[xx], (((1,), (1,)), ((), ())),
                preferred_element_type=f32,
            )
            score = term if score is None else score + term
        allowed = (key_pos <= query_pos) & (key_seg == seg_column[span])
        masked = jnp.where(allowed, score * HD ** (-0.5), NEG_FILL)
        row_max = jnp.max(masked, axis=1, keepdims=True)
        weight = jnp.where(allowed, jnp.exp(masked - row_max), 0.0)
        row_total = jnp.sum(weight, axis=1, keepdims=True)
        rounded = weight.astype(bf16)
        product = [
            jnp.dot(rounded, keys[xx], preferred_element_type=f32) for xx in range(nx)
        ]
        mixed = None
        for xx in reversed(range(nx)):
            low = pltpu.roll(product[xx], (half + xx * quarter) % HD, 1)
            high = pltpu.roll(product[xx], (HD - (nx - 1 - xx) * quarter) % HD, 1)
            lane_block = lane // quarter
            value = jnp.where(lane_block < nx, low, high)
            mixed = value if mixed is None else jnp.where(lane_block % nx == xx, value, mixed)
        mix_own[span, :] = (mixed / row_total).astype(bf16)
        if nz > 3:
            for c in range(b * WO_CHUNKS // nf, (b + 1) * WO_CHUNKS // nf):
                wo_end(2, c)

    head = f * nx + x

    def mix_send(dx, d):
        ff, xx = lax.rem(f + d, nf), lax.rem(x + dx, nx)
        return remote(
            mix_own.at[tile(xx, tok)], mix_buf.at[:, tile(head, HD)],
            s_mix.at[dx, d], r_mix.at[x, f], dev(ff, z, xx),
        )

    def mix_wait(dx, d):
        ff, xx = lax.rem(f + d, nf), lax.rem(x + dx, nx)
        remote(
            mix_own.at[tile(x, tok)], mix_buf.at[:, tile(ff * nx + xx, HD)],
            s_mix.at[dx, d], r_mix.at[xx, ff], here,
        ).wait_recv()

    for pair in pairs[1:]:
        mix_send(*pair).start()
    own_mix = pltpu.make_async_copy(
        mix_own.at[tile(x, tok)], mix_buf.at[:, tile(head, HD)], s_loc.at[6]
    )
    own_mix.start()
    for d in range(3 if nz > 3 else 2, nz - 1):
        for c in range(WO_CHUNKS):
            wo_end(d, c)
    own_mix.wait()
    own_wo.wait()
    for pair in pairs[1:]:
        mix_wait(*pair)
    wo_end(nz - 1, 0)
    for c in range(WO_CHUNKS):
        if c + 1 < WO_CHUNKS:
            wo_end(nz - 1, c + 1)
        for j in range(nz):
            wo_wait(j, other, c)
        out[:, c * chunk : (c + 1) * chunk] = jnp.dot(
            mix_buf[...], wo_buf[:, c * chunk : (c + 1) * chunk], preferred_element_type=f32
        ).astype(bf16)

    hid_send.wait_send()
    seg_same.wait_send()
    for d in range(1, nz):
        wkv_send(d).wait_send()
    for d in range(1, nf):
        kvp_send(d).wait_send()
        q_send(lax.rem(f + d, nf)).wait_send()
    for pair in pairs[1:]:
        kv_send(1, *pair).wait_send()
        mix_send(*pair).wait_send()

    @pl.when(z < nz - 1)
    def _():
        for xx in range(nx):
            seg_next(xx).wait_send()
        kv_next().wait_send()

    @pl.when(z > 0)
    def _():
        for pair in pairs[1:]:
            kv_send(0, *pair).wait_send()

    for j in range(nz):
        for c in range(WO_CHUNKS):
            wo_cross(j, c).wait_send()

        @pl.when((z < nz - 1) & (z >= j))
        def _():
            wq_copy(wq, j, True).wait_send()
            for c in range(WO_CHUNKS):
                wo_copy(j, c, True).wait_send()

        @pl.when((z > 0) & (z <= j))
        def _():
            wq_copy(wq, j, False).wait_send()
            for c in range(WO_CHUNKS):
                wo_copy(j, c, False).wait_send()


def fused_on_device(nf, nz, nx, hidden, w_query, w_keyvalue, w_output, segment_ids):
    tok, kdim = hidden.shape
    cols = w_output.shape[1]
    rows = tok * nx
    sub = rows // nf
    kvw = w_keyvalue.shape[1]
    f32, bf16 = jnp.float32, jnp.bfloat16
    dma = pltpu.SemaphoreType.DMA
    vmem = pl.BlockSpec(memory_space=pltpu.VMEM)
    scratch = [
        pltpu.VMEM((rows, kdim), bf16),
        pltpu.VMEM((nz, kdim, HD), bf16),
        pltpu.VMEM((nz * kvw, kdim), bf16),
        pltpu.VMEM((nz * nx * HD, cols), bf16),
        pltpu.VMEM((2, nx, 1, tok), jnp.int32),
        pltpu.VMEM((nz, rows, HD), f32),
        pltpu.VMEM((nf, rows, HD), f32),
        pltpu.VMEM((rows, nz * kvw), f32),
        pltpu.VMEM((nf, sub, nz * kvw), f32),
        pltpu.VMEM((sub, HD), bf16),
        pltpu.VMEM((2, nx, rows, HD), bf16),
        pltpu.VMEM((rows, HD), bf16),
        pltpu.VMEM((tok, nz * nx * HD), bf16),
        pltpu.VMEM((rows, HD), f32),
        pltpu.VMEM((rows, HD), f32),
        dma((7,)), dma, dma, dma((1 + nx,)), dma((2, nx)),
        dma((nz,)), dma((nz,)), dma((nz,)), dma((nz,)), dma((nz,)),
        dma((nz,)), dma((nf,)), dma((nf,)), dma((nf,)),
        dma((2, nx, nf)), dma((2, nx, nf)),
        dma((nz, WO_CHUNKS)), dma((nz, WO_CHUNKS)), dma((nz, WO_CHUNKS)),
        dma((nz * nx, WO_CHUNKS)), dma((nx, nf)), dma((nx, nf)),
    ]
    return pl.pallas_call(
        functools.partial(fused_kernel, nf, nz, nx),
        out_shape=jax.ShapeDtypeStruct((tok, cols), bf16),
        in_specs=[vmem] * 5,
        out_specs=vmem,
        scratch_shapes=scratch,
        name="fused_sublayer",
        compiler_params=pltpu.CompilerParams(
            collective_id=0, has_side_effects=True, vmem_limit_bytes=60 * 1024 * 1024
        ),
    )(hidden, w_query, w_keyvalue.T, w_output, segment_ids.reshape(1, tok))


def solution(mesh):
    in_specs = (P("sp", "fsdp"), P("fsdp", "sp"), P("fsdp", "sp"), P("sp", "fsdp"), P("sp"))
    out_specs = P("sp", "fsdp")
    nf, sp = mesh.shape["fsdp"], mesh.shape["sp"]
    if sp == GROUP and sp == 2 * nf:
        body = functools.partial(fused_on_device, nf, nf, sp // nf)
    else:
        body = on_device
    return jax.shard_map(
        body, mesh=mesh, in_specs=in_specs, out_specs=out_specs, check_vma=False
    )
```
